256 devices in a mesh: tm: 8 (over x, core), space: 32 (over z, y).
Axes of the slice: x: 4, y: 4, z: 8, core: 2. Of those that a mesh axis runs over, the one named last changes fastest.
Arguments:
- initial_state: float32 [512, 3, 512], P('space'), may hold values from -1 to 1, as said below
- applied_field: float32 [512, 3, 512], P('space'), may hold values from -2 to 2
- coupling: float32 [512, 512], P('space'), may hold values from 0.5 to 2
Outputs:
- slice_states: float32 [8, 512, 3, 512], P('tm', 'space')
The draws below stay inside these ranges and needn't reach their ends.
Inputs may be any that keep to these rules, and one draw needn't show every extreme that they name: `initial_state`: every cell's three components form a vector of length one.
All inputs are finite; a program needn't handle non-finite values.
Results may differ from the reference program's by a relative error of at most 0.00014.
Values sent between devices are 32-bit elements; how exact they have to be, the bound alone decides.
A program may use at most 128 MiB of HBM per device.

```python
import math
import jax
import jax.numpy as jnp

GRID = 512
FINE = 2
ITERS = 1
SLICES = 8


def base_frame(key):
    frame_key = jax.random.fold_in(key, 7)
    sign_key, tilt_key = jax.random.split(frame_key)
    signs = (2 * jax.random.randint(sign_key, (3,), 0, 2) - 1).astype(jnp.float32)
    tilt = jax.random.uniform(tilt_key, (), jnp.float32, 0.6, 0.9)
    return (signs, tilt)


def draw_initial_state(key, part):
    signs, tilt = base_frame(key)
    noise_key = jax.random.fold_in(key, 11)
    in_plane = jnp.cos(tilt) / math.sqrt(2.0)
    base = jnp.stack([signs[0] * in_plane, signs[1] * in_plane, signs[2] * jnp.sin(tilt)]).reshape(1, 3, 1)
    noise = jax.random.uniform(noise_key, (GRID, 3, GRID), jnp.float32, -0.45, 0.45)
    vector = base + noise
    length = jnp.sqrt(jnp.sum(vector * vector, axis=1, keepdims=True))
    return vector / length


def draw_applied_field(key, part):
    signs, tilt = base_frame(key)
    noise_key = jax.random.fold_in(key, 13)
    field_scale = 2.5 / math.sqrt(2.0)
    base = jnp.stack([-signs[1] * field_scale, signs[0] * field_scale, 0.0 * field_scale]).reshape(1, 3, 1)
    noise = 0.4 * jax.random.normal(noise_key, (GRID, 3, GRID), jnp.float32)
    return jnp.clip(base + noise, -2.0, 2.0)


def shard_levels(rng, dims, cuts, low, top_value):
    def one(dim, blocks):
        steps = jax.random.uniform(jax.random.fold_in(jax.random.fold_in(rng, 6), dim), (blocks,), jnp.float32, low / len(cuts), top_value / len(cuts))
        return jnp.repeat(jnp.exp(steps), dims[dim] // blocks).reshape((-1,) + (1,) * (len(dims) - dim - 1))

    gain = one(*cuts[0])
    for cut in cuts[1:]:
        gain = gain * one(*cut)
    return gain


def setup_inputs(seed: int = 0) -> dict:
    arg_keys = jax.random.split(jax.random.key(seed), 4)
    initial_state = draw_initial_state(jax.random.fold_in(arg_keys[3], 71), 0)
    applied_field = draw_applied_field(jax.random.fold_in(arg_keys[3], 71), 0)
    coupling = jnp.clip(jnp.exp(math.log(2.0) - 1.3862944 * jax.random.uniform(arg_keys[2], (GRID, GRID), jnp.float32) ** shard_levels(arg_keys[2], (GRID, GRID), ((0, 32),), -0.2, 0.2)), 0.5, 2.0)
    return dict(initial_state=initial_state, applied_field=applied_field, coupling=coupling)


step_time = 0.06
damping = 0.02
stiffness = 0.25
thickness = 8.0

def spectral_tensor(row_index, column_index, length):
    half_length = length // 2
    signed_rows = jnp.where(row_index < half_length, row_index, row_index - length).astype(jnp.float32)
    signed_columns = jnp.where(column_index < half_length, column_index, column_index - length).astype(jnp.float32)
    wave_rows = 2.0 * math.pi / length * signed_rows[:, None]
    wave_columns = 2.0 * math.pi / length * signed_columns[None, :]
    squared = wave_rows * wave_rows + wave_columns * wave_columns
    nonzero = squared > 0.0
    safe_square = jnp.where(nonzero, squared, 1.0)
    scaled_wave = jnp.sqrt(safe_square) * thickness
    film_factor = jnp.where(nonzero, (1.0 - jnp.exp(-scaled_wave)) / scaled_wave, 1.0)
    in_plane = (1.0 - film_factor) / safe_square
    nyquist = (row_index[:, None] == half_length) | (column_index[None, :] == half_length)
    normalizer = -1.0 / (length * length)
    tensor_first = in_plane * wave_columns * wave_columns * normalizer
    tensor_second = in_plane * wave_rows * wave_rows * normalizer
    tensor_cross = jnp.where(nyquist, 0.0, in_plane * wave_columns * wave_rows) * normalizer
    tensor_normal = film_factor * normalizer
    return (tensor_first, tensor_second, tensor_cross, tensor_normal)

def exchange_field(padded_state, padded_coupling):
    center_state = padded_state[1:-1]
    center_coupling = padded_coupling[1:-1]
    wide_state = jnp.pad(padded_state, ((0, 0), (0, 0), (1, 1)))
    wide_coupling = jnp.pad(padded_coupling, ((0, 0), (1, 1)))
    neighbour_sum = padded_coupling[2:, None, :] * (padded_state[2:] - center_state)
    neighbour_sum = neighbour_sum + padded_coupling[:-2, None, :] * (padded_state[:-2] - center_state)
    neighbour_sum = neighbour_sum + wide_coupling[1:-1, None, 2:] * (wide_state[1:-1, :, 2:] - center_state)
    neighbour_sum = neighbour_sum + wide_coupling[1:-1, None, :-2] * (wide_state[1:-1, :, :-2] - center_state)
    return stiffness * center_coupling[:, None, :] * neighbour_sum

def torque(magnet, effective):
    first_cross = jnp.cross(magnet, effective, axis=1)
    second_cross = jnp.cross(magnet, first_cross, axis=1)
    return -(first_cross + damping * second_cross) / (1.0 + damping * damping)

def demag_field(magnet):
    padded = jnp.pad(magnet, ((0, GRID), (0, 0), (0, GRID)))
    spectrum = jnp.fft.fft2(padded, axes=(0, 2))
    index_all = jnp.arange(2 * GRID, dtype=jnp.int32)
    tensor_first, tensor_second, tensor_cross, tensor_normal = spectral_tensor(index_all, index_all, 2 * GRID)
    first_out = tensor_first * spectrum[:, 0] + tensor_cross * spectrum[:, 1]
    second_out = tensor_cross * spectrum[:, 0] + tensor_second * spectrum[:, 1]
    third_out = tensor_normal * spectrum[:, 2]
    combined = jnp.stack([first_out, second_out, third_out], axis=1)
    result = jnp.fft.ifft2(combined, axes=(0, 2)) * float(2 * GRID * (2 * GRID))
    return jnp.real(result)[:GRID, :, :GRID].astype(jnp.float32)

def effective_fine(magnet, applied_field, padded_coupling):
    padded_state = jnp.pad(magnet, ((1, 1), (0, 0), (0, 0)))
    return exchange_field(padded_state, padded_coupling) + demag_field(magnet) + applied_field

def propagate_fine(magnet, applied_field, padded_coupling):
    for repeat in range(FINE):
        first_rate = torque(magnet, effective_fine(magnet, applied_field, padded_coupling))
        predicted = magnet + step_time * first_rate
        second_rate = torque(predicted, effective_fine(predicted, applied_field, padded_coupling))
        magnet = magnet + 0.5 * step_time * (first_rate + second_rate)
    return magnet

def propagate_coarse(magnet, applied_field, padded_coupling):
    padded_state = jnp.pad(magnet, ((1, 1), (0, 0), (0, 0)))
    local_demag = jnp.array([0.0, 0.0, -1.0], dtype=jnp.float32).reshape(1, 3, 1)
    effective = exchange_field(padded_state, padded_coupling) + applied_field + magnet * local_demag
    return magnet + FINE * step_time * torque(magnet, effective)

def coarse_sweep(differences, initial_state, applied_field, padded_coupling):
    current = initial_state
    starts = []
    coarse_ends = []
    slice_ends = []
    for slice_number in range(SLICES):
        predicted = propagate_coarse(current, applied_field, padded_coupling)
        advanced = predicted + differences[slice_number]
        starts.append(current)
        coarse_ends.append(predicted)
        slice_ends.append(advanced)
        current = advanced
    return (starts, coarse_ends, slice_ends)

def reference(initial_state, applied_field, coupling):
    padded_coupling = jnp.pad(coupling, ((1, 1), (0, 0)))
    differences = [jnp.zeros_like(initial_state) for slice_number in range(SLICES)]
    starts, coarse_ends, slice_ends = coarse_sweep(differences, initial_state, applied_field, padded_coupling)
    for iteration in range(ITERS):
        differences = [propagate_fine(starts[slice_number], applied_field, padded_coupling) - coarse_ends[slice_number] for slice_number in range(SLICES)]
        starts, coarse_ends, slice_ends = coarse_sweep(differences, initial_state, applied_field, padded_coupling)
    return jnp.stack(slice_ends, axis=0)
```

```python
import math

import jax
import jax.numpy as jnp
import numpy as np
from jax import lax
from jax.experimental import pallas as pl
from jax.experimental.pallas import tpu as pltpu
from jax.sharding import PartitionSpec as P

MESH = pl.DeviceIdType.MESH
F32 = jnp.float32
BF16 = jnp.bfloat16

FINE = 2
step_time = 0.06
damping = 0.02
stiffness = 0.25
thickness = 8.0

GRID = 512
LENGTH = 2 * GRID
ROWS = 16
SPACE = 32
TM = 8
WORKERS = 24
PAIRED = 16


def twiddle_tables():
    unit = 2.0 * np.pi / LENGTH
    col = np.arange(LENGTH)
    wave = 32 * (col // 64) + col % 32
    kind = (col // 32) % 2
    phase = np.where(kind == 1, np.pi / 2, 0.0)
    nyquist = (kind == 1) & (wave == 0)
    wave = np.where(nyquist, GRID, wave)
    phase = np.where(nyquist, 0.0, phase)
    coarse = 16 * np.arange(GRID // 16)[:, None]
    fine = np.arange(16)[:, None]
    angle_coarse = unit * (coarse * wave % LENGTH)
    angle_fine = unit * (fine * wave % LENGTH) + phase
    x = np.arange(GRID)[None, :]
    block = 32 * np.arange(GRID // 32)[:, None]
    inner = np.arange(64)[:, None]
    angle_block = unit * (block * x % LENGTH)
    angle_inner = unit * (inner % 32 * x % LENGTH) + np.where(inner >= 32, np.pi / 2, 0.0)

    def both(angle):
        return np.concatenate([np.cos(angle), np.sin(angle)], axis=0).astype(np.float32)

    return both(angle_coarse), both(angle_fine), both(angle_block), both(angle_inner)


def split(value):
    high = value.astype(BF16)
    return high, (value - high.astype(F32)).astype(BF16)


def dot(left, right):
    return jnp.dot(left, right, preferred_element_type=F32)


def cross(a, b):
    return [
        a[1] * b[2] - a[2] * b[1],
        a[2] * b[0] - a[0] * b[2],
        a[0] * b[1] - a[1] * b[0],
    ]


def torque(magnet, effective):
    first = cross(magnet, effective)
    second = cross(magnet, first)
    scale = -1.0 / (1.0 + damping * damping)
    return [scale * (f + damping * s) for f, s in zip(first, second)]


def kernel(
    state_in, field_in, coupling_in, t_coarse, t_fine, t_block, t_inner, out,
    state, field, coupling, weights, e1_high, e1_low, e2_high, e2_low, diagonal, cross_term,
    outgoing, columns, mixed, answer, returned, edges, edge_in, base, slope, local_field, coarse_end, jumps,
    halo_send, halo_recv, edge_send, edge_recv, out_send, out_recv, back_send, back_recv,
    jump_send, jump_recv, gather_send, gather_recv, forward_send,
):
    slice_index = lax.axis_index("tm")
    place = lax.axis_index("space")
    chip = slice_index // 2
    core = slice_index % 2
    above = (place + SPACE - 1) % SPACE
    below = (place + 1) % SPACE
    offset = (place % 4 - (place // 4) % 4 + 3) % 4
    rank = 3 * (place // 4) + offset
    works = offset < 3
    rank = jnp.minimum(rank, WORKERS - 1)

    def worker_place(worker):
        z = worker // 3
        return 4 * z + (z + 1 + worker % 3) % 4

    barrier = pltpu.get_barrier_semaphore()

    def greet_space(i, carry):
        pl.semaphore_signal(barrier, inc=1, device_id=(slice_index, (place + i) % SPACE), device_id_type=MESH)
        return carry

    def greet_tm(i, carry):
        pl.semaphore_signal(barrier, inc=1, device_id=((slice_index + i) % TM, place), device_id_type=MESH)
        return carry

    lax.fori_loop(1, SPACE, greet_space, 0)
    lax.fori_loop(1, TM, greet_tm, 0)

    zero_rows = jnp.zeros((8, GRID), F32)
    for c in range(3):
        for slot in range(3):
            state[slot, c, 0:8, :] = zero_rows
            state[slot, c, 40:48, :] = zero_rows
        state[2, c, 16:32, :] = state_in[:, c, :]
        field[c, 8:24, :] = field_in[:, c, :]
    coupling[0:8, :] = zero_rows
    coupling[40:48, :] = zero_rows
    coupling[16:32, :] = coupling_in[...]
    edges[...] = zero_rows

    def build_e1(a, carry):
        value = t_coarse[pl.ds(a, 1), :] * t_fine[0:16, :] - t_coarse[pl.ds(32 + a, 1), :] * t_fine[16:32, :]
        high, low = split(value)
        rows = pl.ds(pl.multiple_of(16 * a, 16), 16)
        e1_high[rows, :] = high
        e1_low[rows, :] = low
        return carry

    lax.fori_loop(0, GRID // 16, build_e1, 0)
    inner_row = lax.broadcasted_iota(jnp.int32, (64, GRID), 0)
    inner_lane = lax.broadcasted_iota(jnp.int32, (64, GRID), 1)
    alternating = (1 - 2 * (inner_lane % 2)).astype(F32)

    def build_e2(j, carry):
        value = t_block[pl.ds(j, 1), :] * t_inner[0:64, :] - t_block[pl.ds(16 + j, 1), :] * t_inner[64:128, :]
        value = jnp.where((inner_row == 32) & (j == 0), alternating, value)
        high, low = split(value)
        rows = pl.ds(pl.multiple_of(64 * j, 64), 64)
        e2_high[rows, :] = high
        e2_low[rows, :] = low
        return carry

    lax.fori_loop(0, GRID // 32, build_e2, 0)

    pl.semaphore_wait(barrier, SPACE - 1 + TM - 1)

    def halo_copies():
        copies = []
        for side, target, source_row, landing_row in ((0, below, 24, 8), (1, above, 16, 32)):
            for what, (source, landing) in enumerate(
                (
                    (state.at[2, :, pl.ds(source_row, 8), :], state.at[2, :, pl.ds(landing_row, 8), :]),
                    (field.at[:, pl.ds(source_row - 8, 8), :], field.at[:, pl.ds(landing_row - 8, 8), :]),
                    (coupling.at[pl.ds(source_row, 8), :], coupling.at[pl.ds(landing_row, 8), :]),
                )
            ):
                copies.append(
                    pltpu.make_async_remote_copy(
                        src_ref=source, dst_ref=landing,
                        send_sem=halo_send.at[side, what], recv_sem=halo_recv.at[side, what],
                        device_id=(slice_index, target), device_id_type=MESH,
                    )
                )
        return copies

    first_halo = halo_copies()
    for copy in first_halo:
        copy.start()

    def build_tensor(chunk, carry):
        row = 256 * chunk + lax.broadcasted_iota(jnp.int32, (256, 128), 0)
        lane = lax.broadcasted_iota(jnp.int32, (256, 128), 1)
        quarter = lane // 32
        paired = rank < PAIRED
        wave_y = 32 * (row // 64) + row % 32
        wave_y = jnp.where((wave_y == 0) & ((row // 32) % 2 == 1), GRID, wave_y)
        first_x = jnp.where(paired, 32 * rank, 64 * (rank - PAIRED) + 32 * (quarter // 2))
        wave_x = first_x + lane % 32
        wave_x = jnp.where((wave_x == 0) & (quarter % 2 == 1), GRID, wave_x)
        edge_x = (wave_x == 0) | (wave_x == GRID)
        edge_y = (wave_y == 0) | (wave_y == GRID)
        factor = jnp.where(edge_x, 1.0, 2.0) * jnp.where(edge_y, 1.0, 2.0) * (-1.0 / (LENGTH * LENGTH))
        q_x = wave_x.astype(F32) * (2.0 * math.pi / LENGTH)
        q_y = wave_y.astype(F32) * (2.0 * math.pi / LENGTH)
        squared = q_x * q_x + q_y * q_y
        nonzero = (wave_x + wave_y) > 0
        safe = jnp.where(nonzero, squared, 1.0)
        scaled = jnp.sqrt(safe) * thickness
        film = jnp.where(nonzero, (1.0 - jnp.exp(-scaled)) / scaled, 1.0)
        in_plane = (1.0 - film) / safe
        own_wave = jnp.where(quarter < 2, q_x, q_y)
        diag = jnp.where(paired, in_plane * own_wave * own_wave, film)
        sign = jnp.where(quarter % 2 == 0, -1.0, 1.0)
        mix = jnp.where(edge_x | edge_y | jnp.logical_not(paired), 0.0, sign * in_plane * q_x * q_y)
        diagonal[pl.ds(pl.multiple_of(256 * chunk, 256), 256), :] = diag * factor
        mix = (mix * factor).reshape(4, 2, 32, 128)[:, 0].reshape(128, 128)
        cross_term[pl.ds(pl.multiple_of(128 * chunk, 128), 128), :] = mix
        return carry

    lax.fori_loop(0, 4, build_tensor, 0)

    for copy in first_halo:
        copy.wait()
    coupling[8:16, :] = jnp.where(place > 0, coupling[8:16, :], 0.0)
    coupling[32:40, :] = jnp.where(place < SPACE - 1, coupling[32:40, :], 0.0)

    film_lane = lax.broadcasted_iota(jnp.int32, (8, GRID), 1)
    for g in range(4):
        top = 8 + 8 * g
        mid = coupling[top : top + 8, :]
        scaled = stiffness * mid
        up = scaled * coupling[top - 1 : top + 7, :]
        down = scaled * coupling[top + 1 : top + 9, :]
        left = jnp.where(film_lane == 0, 0.0, scaled * pltpu.roll(mid, 1, 1))
        right = jnp.where(film_lane == GRID - 1, 0.0, scaled * pltpu.roll(mid, GRID - 1, 1))
        rows = slice(8 * g, 8 * g + 8)
        weights[0, rows, :] = up
        weights[1, rows, :] = down
        weights[2, rows, :] = left
        weights[3, rows, :] = right
        weights[4, rows, :] = (up + down) + (left + right)

    def exchange(slot, g):
        top = 8 + 8 * g
        rows = slice(8 * g, 8 * g + 8)
        w = [weights[k, rows, :] for k in range(5)]
        magnet, result = [], []
        for c in range(3):
            mid = state[slot, c, top : top + 8, :]
            total = w[0] * state[slot, c, top - 1 : top + 7, :]
            total = total + w[1] * state[slot, c, top + 1 : top + 9, :]
            total = total + w[2] * pltpu.roll(mid, 1, 1)
            total = total + w[3] * pltpu.roll(mid, GRID - 1, 1)
            magnet.append(mid)
            result.append(total - w[4] * mid)
        return magnet, result

    def coarse_group(slot, g):
        magnet, effective = exchange(slot, g)
        rows = slice(8 * g, 8 * g + 8)
        effective = [effective[c] + field[c, rows, :] for c in range(3)]
        effective[2] = effective[2] - magnet[2]
        rate = torque(magnet, effective)
        return [magnet[c] + (FINE * step_time) * rate[c] for c in range(3)]

    def source_slot(n):
        return jnp.where(n == 0, 2, n % 2)

    def first_sweep(n, carry):
        for g in range(4):
            new = coarse_group(source_slot(n), g)
            for c in range(3):
                state[(n + 1) % 2, c, 8 + 8 * g : 16 + 8 * g, :] = new[c]
        return carry

    lax.fori_loop(0, slice_index, first_sweep, 0)
    start_slot = source_slot(slice_index)
    for g in (1, 2):
        new = coarse_group(start_slot, g)
        for c in range(3):
            coarse_end[c, 8 * g - 8 : 8 * g, :] = new[c]
    for c in range(3):
        start = state[start_slot, c, 16:32, :]
        base[c, :, :] = start
        slope[c, :, :] = jnp.zeros_like(start)
        state[0, c, 16:32, :] = start

    low_half = lax.broadcasted_iota(jnp.int32, (ROWS, 128), 1) < 64
    even_quarter = (lax.broadcasted_iota(jnp.int32, (128, 128), 1) // 32) % 2 == 0

    def partner(value):
        return jnp.where(even_quarter, pltpu.roll(value, 32, 1), pltpu.roll(value, 96, 1))

    def send_column(worker):
        return pltpu.make_async_remote_copy(
            src_ref=outgoing.at[worker],
            dst_ref=columns.at[pl.ds(pl.multiple_of(ROWS * place, ROWS), ROWS), :],
            send_sem=out_send, recv_sem=out_recv,
            device_id=(slice_index, worker_place(worker)), device_id_type=MESH,
        )

    def send_back(target):
        return pltpu.make_async_remote_copy(
            src_ref=answer.at[pl.ds(pl.multiple_of(ROWS * target, ROWS), ROWS), :],
            dst_ref=returned.at[rank],
            send_sem=back_send, recv_sem=back_recv,
            device_id=(slice_index, target), device_id_type=MESH,
        )

    def wait_bytes(ref, semaphore):
        pltpu.make_async_copy(ref, ref, semaphore).wait()

    def evaluation(e, carry):
        slot = e % 2
        for c in range(3):
            edges[c : c + 1, :] = state[0, c, 16:17, :]
            edges[3 + c : 4 + c, :] = state[0, c, 31:32, :]
        edge_copies = [
            pltpu.make_async_remote_copy(
                src_ref=edges, dst_ref=edge_in.at[slot, side],
                send_sem=edge_send.at[side], recv_sem=edge_recv.at[slot, side],
                device_id=(slice_index, target), device_id_type=MESH,
            )
            for side, target in ((0, below), (1, above))
        ]
        for copy in edge_copies:
            copy.start()

        magnet = jnp.concatenate([state[0, c, 16:32, :] for c in range(3)], axis=0)
        high, low = split(magnet)
        stacked = jnp.concatenate([high, low], axis=0)
        for part in range(4):
            cols = slice(256 * part, 256 * part + 256)
            wide = dot(stacked, e1_high[:, cols])
            spectrum = wide[0:48] + wide[48:96] + dot(high, e1_low[:, cols])
            for half in range(2):
                t = 2 * part + half
                lanes = slice(128 * half, 128 * half + 128)
                mx, my, mz = spectrum[0:16, lanes], spectrum[16:32, lanes], spectrum[32:48, lanes]
                outgoing[2 * t] = jnp.where(low_half, mx, pltpu.roll(my, 64, 1))
                outgoing[2 * t + 1] = jnp.where(low_half, pltpu.roll(mx, 64, 1), my)
                outgoing[PAIRED + t] = mz

        def start_column(i, inner):
            worker = (rank + i) % WORKERS

            @pl.when(worker_place(worker) != place)
            def _():
                send_column(worker).start()

            return inner

        lax.fori_loop(0, WORKERS, start_column, 0)

        @pl.when(works)
        def _():
            columns[pl.ds(pl.multiple_of(ROWS * place, ROWS), ROWS), :] = outgoing[rank]

        for copy in edge_copies:
            copy.wait()
        for c in range(3):
            state[0, c, 15:16, :] = edge_in[slot, 0, 3 + c : 4 + c, :]
            state[0, c, 32:33, :] = edge_in[slot, 1, c : c + 1, :]
        for g in (1, 2):
            _, effective = exchange(0, g)
            for c in range(3):
                local_field[c, 8 * g - 8 : 8 * g, :] = effective[c] + field[c, 8 * g : 8 * g + 8, :]

        @pl.when(works)
        def _():
            wait_bytes(columns.at[pl.ds(0, ROWS * (SPACE - 1)), :], out_recv)
            column_high, column_low = split(columns[...])
            column_both = jnp.concatenate([column_high, column_low], axis=1)
            for part in range(4):
                rows = slice(256 * part, 256 * part + 256)
                wide = dot(e2_high[rows, :], column_both)
                spectrum = wide[:, 0:128] + wide[:, 128:256] + dot(e2_low[rows, :], column_high)
                spectrum = spectrum.reshape(4, 2, 32, 128)
                real = spectrum[:, 0].reshape(128, 128)
                imag = spectrum[:, 1].reshape(128, 128)
                diag = diagonal[rows, :].reshape(4, 2, 32, 128)
                mix = cross_term[128 * part : 128 * part + 128, :]
                real_out = diag[:, 0].reshape(128, 128) * real + mix * partner(imag)
                imag_out = diag[:, 1].reshape(128, 128) * imag - mix * partner(real)
                both = jnp.stack(
                    [real_out.reshape(4, 32, 128), imag_out.reshape(4, 32, 128)], axis=1
                ).reshape(256, 128)
                both_high, both_low = split(both)
                mixed[rows, 0:128] = both_high
                mixed[rows, 128:256] = both_low
            for part in range(4):
                rows = slice(128 * part, 128 * part + 128)
                wide = dot(e1_high[rows, :], mixed[...])
                answer[rows, :] = wide[:, 0:128] + wide[:, 128:256] + dot(e1_low[rows, :], mixed[:, 0:128])

                def start_back(i, inner, part=part):
                    target = 8 * part + i

                    @pl.when(target != place)
                    def _():
                        send_back(target).start()

                    return inner

                lax.fori_loop(0, 8, start_back, 0)
            returned[rank] = answer[pl.ds(pl.multiple_of(ROWS * place, ROWS), ROWS), :]
            wait_bytes(outgoing.at[pl.ds(0, WORKERS - 1)], out_send)
            wait_bytes(returned.at[pl.ds(0, WORKERS - 1)], back_recv)

        @pl.when(jnp.logical_not(works))
        def _():
            wait_bytes(outgoing, out_send)
            wait_bytes(returned, back_recv)

        parts = [[], [], []]
        for t in range(8):
            first, second = returned[2 * t], returned[2 * t + 1]
            parts[0].append(jnp.where(low_half, first, pltpu.roll(second, 64, 1)))
            parts[1].append(jnp.where(low_half, pltpu.roll(first, 64, 1), second))
            parts[2].append(returned[PAIRED + t])
        spectrum = jnp.concatenate([jnp.concatenate(part, axis=1) for part in parts], axis=0)
        spectrum_high, spectrum_low = split(spectrum)
        wide = dot(jnp.concatenate([spectrum_high, spectrum_low], axis=0), e2_high[...])
        demag = wide[0:48] + wide[48:96] + dot(spectrum_high, e2_low[...])

        corrects = slot == 1
        length = jnp.where(corrects, 0.5 * step_time, step_time)
        for g in range(2):
            rows = slice(8 * g, 8 * g + 8)
            here = [state[0, c, 16 + 8 * g : 24 + 8 * g, :] for c in range(3)]
            effective = [local_field[c, rows, :] + demag[16 * c + 8 * g : 16 * c + 8 * g + 8] for c in range(3)]
            rate = torque(here, effective)
            for c in range(3):
                start = base[c, rows, :]
                new = start + length * (slope[c, rows, :] + rate[c])
                state[0, c, 16 + 8 * g : 24 + 8 * g, :] = new
                slope[c, rows, :] = jnp.where(corrects, 0.0, rate[c])
                base[c, rows, :] = jnp.where(corrects, new, start)

        @pl.when(works)
        def _():
            wait_bytes(answer.at[pl.ds(0, ROWS * (SPACE - 1)), :], back_send)

        return carry

    lax.fori_loop(0, 2 * FINE, evaluation, 0)

    for c in range(3):
        jumps[slice_index, c, 8:24, :] = state[0, c, 16:32, :] - coarse_end[c, :, :]
    jump_halo = [
        pltpu.make_async_remote_copy(
            src_ref=jumps.at[slice_index, :, pl.ds(source_row, 8), :],
            dst_ref=jumps.at[slice_index, :, pl.ds(landing_row, 8), :],
            send_sem=jump_send.at[side], recv_sem=jump_recv.at[side],
            device_id=(slice_index, target), device_id_type=MESH,
        )
        for side, target, source_row, landing_row in ((0, below, 16, 0), (1, above, 8, 24))
    ]
    for copy in jump_halo:
        copy.start()
    for copy in jump_halo:
        copy.wait()

    def send_jump(n, target, semaphore):
        return pltpu.make_async_remote_copy(
            src_ref=jumps.at[n], dst_ref=jumps.at[n],
            send_sem=semaphore, recv_sem=gather_recv.at[n],
            device_id=(target, place), device_id_type=MESH,
        )

    mate = slice_index + 1 - 2 * core

    @pl.when(core == 0)
    def _():
        send_jump(slice_index, mate, gather_send.at[0]).start()

    for i in (1, 2, 3):

        @pl.when(chip + i < TM // 2)
        def _(i=i):
            send_jump(slice_index, slice_index + 2 * i, gather_send.at[i]).start()

    def second_sweep(n, carry):
        @pl.when(n < slice_index)
        def _():
            wait_bytes(jumps.at[n], gather_recv.at[n])

        @pl.when((n < slice_index) & (n % 2 == core))
        def _():
            send_jump(n, mate, forward_send.at[n]).start()

        for g in range(4):
            new = coarse_group(source_slot(n), g)
            for c in range(3):
                state[(n + 1) % 2, c, 8 + 8 * g : 16 + 8 * g, :] = new[c] + jumps[n, c, 8 * g : 8 * g + 8, :]
        return carry

    lax.fori_loop(0, slice_index + 1, second_sweep, 0)
    for c in range(3):
        out[0, :, c, :] = state[(slice_index + 1) % 2, c, 16:32, :]

    def finish_forward(n, carry):
        @pl.when(n % 2 == core)
        def _():
            wait_bytes(jumps.at[n], forward_send.at[n])

        return carry

    lax.fori_loop(0, slice_index, finish_forward, 0)

    @pl.when(core == 0)
    def _():
        wait_bytes(jumps.at[slice_index], gather_send.at[0])

    for i in (1, 2, 3):

        @pl.when(chip + i < TM // 2)
        def _(i=i):
            wait_bytes(jumps.at[slice_index], gather_send.at[i])


def solution(mesh):
    tables = twiddle_tables()
    vmem = pltpu.VMEM
    dma = pltpu.SemaphoreType.DMA
    scratch = [
        vmem((3, 3, 48, GRID), F32),
        vmem((3, 32, GRID), F32),
        vmem((48, GRID), F32),
        vmem((5, 32, GRID), F32),
        vmem((GRID, LENGTH), BF16),
        vmem((GRID, LENGTH), BF16),
        vmem((LENGTH, GRID), BF16),
        vmem((LENGTH, GRID), BF16),
        vmem((LENGTH, 128), F32),
        vmem((GRID, 128), F32),
        vmem((WORKERS, ROWS, 128), F32),
        vmem((GRID, 128), F32),
        vmem((LENGTH, 256), BF16),
        vmem((GRID, 128), F32),
        vmem((WORKERS, ROWS, 128), F32),
        vmem((8, GRID), F32),
        vmem((2, 2, 8, GRID), F32),
        vmem((3, ROWS, GRID), F32),
        vmem((3, ROWS, GRID), F32),
        vmem((3, ROWS, GRID), F32),
        vmem((3, ROWS, GRID), F32),
        vmem((TM, 3, 32, GRID), F32),
        dma((2, 3)),
        dma((2, 3)),
        dma((2,)),
        dma((2, 2)),
        dma,
        dma,
        dma,
        dma,
        dma((2,)),
        dma((2,)),
        dma((4,)),
        dma((TM,)),
        dma((TM,)),
    ]

    def shards(initial_state, applied_field, coupling):
        return pl.pallas_call(
            kernel,
            out_shape=jax.ShapeDtypeStruct((1, ROWS, 3, GRID), F32),
            in_specs=[pl.BlockSpec(memory_space=pltpu.VMEM)] * 7,
            out_specs=pl.BlockSpec(memory_space=pltpu.VMEM),
            scratch_shapes=scratch,
            compiler_params=pltpu.CompilerParams(collective_id=0, has_side_effects=True),
        )(initial_state, applied_field, coupling, *[jnp.asarray(table) for table in tables])

    return jax.shard_map(
        shards,
        mesh=mesh,
        in_specs=(P("space", None, None), P("space", None, None), P("space", None)),
        out_specs=P("tm", "space", None, None),
        check_vma=False,
    )
```

```python
import math

import jax
import jax.numpy as jnp
import numpy as np
from jax import lax
from jax.experimental import pallas as pl
from jax.experimental.pallas import tpu as pltpu
from jax.sharding import PartitionSpec as P

MESH = pl.DeviceIdType.MESH
F32 = jnp.float32
BF16 = jnp.bfloat16

FINE = 2
step_time = 0.06
damping = 0.02
stiffness = 0.25
thickness = 8.0

GRID = 512
LENGTH = 2 * GRID
ROWS = 16
SPACE = 32
TM = 8
WORKERS = 24
PAIRED = 16


def send_order():
    order = []
    for far in (4, 3, 2, 1, 0):
        for dy in (2, 1, -1, 0):
            for dz in (far, -far) if far in (1, 2, 3) else (far,):
                order.append((dz, dy if dz >= 0 else -dy))
    return [pair for pair in order if pair != (0, 0)]


def twiddle_tables():
    unit = 2.0 * np.pi / LENGTH
    col = np.arange(LENGTH)
    wave = 32 * (col // 64) + col % 32
    kind = (col // 32) % 2
    phase = np.where(kind == 1, np.pi / 2, 0.0)
    nyquist = (kind == 1) & (wave == 0)
    wave = np.where(nyquist, GRID, wave)
    phase = np.where(nyquist, 0.0, phase)
    coarse = 16 * np.arange(GRID // 16)[:, None]
    fine = np.arange(16)[:, None]
    angle_coarse = unit * (coarse * wave % LENGTH)
    angle_fine = unit * (fine * wave % LENGTH) + phase
    x = np.arange(GRID)[None, :]
    block = 32 * np.arange(GRID // 32)[:, None]
    inner = np.arange(64)[:, None]
    angle_block = unit * (block * x % LENGTH)
    angle_inner = unit * (inner % 32 * x % LENGTH) + np.where(inner >= 32, np.pi / 2, 0.0)

    def both(angle):
        return np.concatenate([np.cos(angle), np.sin(angle)], axis=0).astype(np.float32)

    return both(angle_coarse), both(angle_fine), both(angle_block), both(angle_inner)


def split(value):
    high = value.astype(BF16)
    return high, (value - high.astype(F32)).astype(BF16)


def dot(left, right):
    return jnp.dot(left, right, preferred_element_type=F32)


def cross(a, b):
    return [
        a[1] * b[2] - a[2] * b[1],
        a[2] * b[0] - a[0] * b[2],
        a[0] * b[1] - a[1] * b[0],
    ]


def torque(magnet, effective):
    first = cross(magnet, effective)
    second = cross(magnet, first)
    scale = -1.0 / (1.0 + damping * damping)
    return [scale * (f + damping * s) for f, s in zip(first, second)]


def kernel(
    state_in, field_in, coupling_in, t_coarse, t_fine, t_block, t_inner, out,
    state, field, coupling, weights, e1_high, e1_low, e2_high, e2_low, diagonal, cross_term,
    outgoing, columns, mixed, answer, returned, edges, edge_in, base, slope, local_field, coarse_end, jumps,
    halo_send, halo_recv, edge_send, edge_recv, out_send, out_recv, back_send, back_recv,
    jump_send, jump_recv, gather_send, gather_recv, forward_send,
):
    slice_index = lax.axis_index("tm")
    place = lax.axis_index("space")

    def device(which_slice, which_place):
        return (which_slice, which_place)

    chip = slice_index // 2
    core = slice_index % 2
    above = (place + SPACE - 1) % SPACE
    below = (place + 1) % SPACE
    offset = (place % 4 - (place // 4) % 4 + 3) % 4
    rank = 3 * (place // 4) + offset
    works = offset < 3
    rank = jnp.minimum(rank, WORKERS - 1)

    place_z, place_y = place // 4, place % 4

    def at(dz, dy):
        return 4 * ((place_z + dz) % 8) + (place_y + dy) % 4

    barrier = pltpu.get_barrier_semaphore()

    def greet_space(i, carry):
        pl.semaphore_signal(barrier, inc=1, device_id=device(slice_index, (place + i) % SPACE), device_id_type=MESH)
        return carry

    def greet_tm(i, carry):
        pl.semaphore_signal(barrier, inc=1, device_id=device((slice_index + i) % TM, place), device_id_type=MESH)
        return carry

    lax.fori_loop(1, SPACE, greet_space, 0)
    lax.fori_loop(1, TM, greet_tm, 0)

    zero_rows = jnp.zeros((8, GRID), F32)
    for c in range(3):
        for slot in range(3):
            state[slot, c, 0:8, :] = zero_rows
            state[slot, c, 40:48, :] = zero_rows
        state[2, c, 16:32, :] = state_in[c]
        field[c, 8:24, :] = field_in[c]
    coupling[0:8, :] = zero_rows
    coupling[40:48, :] = zero_rows
    coupling[16:32, :] = coupling_in[...]
    edges[...] = zero_rows

    pl.semaphore_wait(barrier, SPACE - 1 + TM - 1)

    def halo_copies():
        copies = []
        for side, target, source_row, landing_row in ((0, below, 24, 8), (1, above, 16, 32)):
            for what, (source, landing) in enumerate(
                (
                    (state.at[2, :, pl.ds(source_row, 8), :], state.at[2, :, pl.ds(landing_row, 8), :]),
                    (field.at[:, pl.ds(source_row - 8, 8), :], field.at[:, pl.ds(landing_row - 8, 8), :]),
                    (coupling.at[pl.ds(source_row, 8), :], coupling.at[pl.ds(landing_row, 8), :]),
                )
            ):
                copies.append(
                    pltpu.make_async_remote_copy(
                        src_ref=source, dst_ref=landing,
                        send_sem=halo_send.at[side, what], recv_sem=halo_recv.at[side, what],
                        device_id=device(slice_index, target), device_id_type=MESH,
                    )
                )
        return copies

    first_halo = halo_copies()
    for copy in first_halo:
        copy.start()

    def build_e1(a, carry):
        value = t_coarse[pl.ds(a, 1), :] * t_fine[0:16, :] - t_coarse[pl.ds(32 + a, 1), :] * t_fine[16:32, :]
        high, low = split(value)
        rows = pl.ds(pl.multiple_of(16 * a, 16), 16)
        e1_high[rows, :] = high
        e1_low[rows, :] = low
        return carry

    lax.fori_loop(0, GRID // 16, build_e1, 0)
    inner_row = lax.broadcasted_iota(jnp.int32, (64, GRID), 0)
    inner_lane = lax.broadcasted_iota(jnp.int32, (64, GRID), 1)
    alternating = (1 - 2 * (inner_lane % 2)).astype(F32)

    def build_e2(j, carry):
        value = t_block[pl.ds(j, 1), :] * t_inner[0:64, :] - t_block[pl.ds(16 + j, 1), :] * t_inner[64:128, :]
        value = jnp.where((inner_row == 32) & (j == 0), alternating, value)
        high, low = split(value)
        rows = pl.ds(pl.multiple_of(64 * j, 64), 64)
        e2_high[rows, :] = high
        e2_low[rows, :] = low
        return carry

    lax.fori_loop(0, GRID // 32, build_e2, 0)

    def build_tensor(chunk, carry):
        row = 256 * chunk + lax.broadcasted_iota(jnp.int32, (256, 128), 0)
        lane = lax.broadcasted_iota(jnp.int32, (256, 128), 1)
        quarter = lane // 32
        paired = rank < PAIRED
        wave_y = 32 * (row // 64) + row % 32
        wave_y = jnp.where((wave_y == 0) & ((row // 32) % 2 == 1), GRID, wave_y)
        first_x = jnp.where(paired, 32 * rank, 64 * (rank - PAIRED) + 32 * (quarter // 2))
        wave_x = first_x + lane % 32
        wave_x = jnp.where((wave_x == 0) & (quarter % 2 == 1), GRID, wave_x)
        edge_x = (wave_x == 0) | (wave_x == GRID)
        edge_y = (wave_y == 0) | (wave_y == GRID)
        factor = jnp.where(edge_x, 1.0, 2.0) * jnp.where(edge_y, 1.0, 2.0) * (-1.0 / (LENGTH * LENGTH))
        q_x = wave_x.astype(F32) * (2.0 * math.pi / LENGTH)
        q_y = wave_y.astype(F32) * (2.0 * math.pi / LENGTH)
        squared = q_x * q_x + q_y * q_y
        nonzero = (wave_x + wave_y) > 0
        safe = jnp.where(nonzero, squared, 1.0)
        scaled = jnp.sqrt(safe) * thickness
        film = jnp.where(nonzero, (1.0 - jnp.exp(-scaled)) / scaled, 1.0)
        in_plane = (1.0 - film) / safe
        own_wave = jnp.where(quarter < 2, q_x, q_y)
        diag = jnp.where(paired, in_plane * own_wave * own_wave, film)
        sign = jnp.where(quarter % 2 == 0, -1.0, 1.0)
        mix = jnp.where(edge_x | edge_y | jnp.logical_not(paired), 0.0, sign * in_plane * q_x * q_y)
        diagonal[pl.ds(pl.multiple_of(256 * chunk, 256), 256), :] = diag * factor
        mix = (mix * factor).reshape(4, 2, 32, 128)[:, 0].reshape(128, 128)
        cross_term[pl.ds(pl.multiple_of(128 * chunk, 128), 128), :] = mix
        return carry

    lax.fori_loop(0, 4, build_tensor, 0)

    for copy in first_halo:
        copy.wait()
    coupling[8:16, :] = jnp.where(place > 0, coupling[8:16, :], 0.0)
    coupling[32:40, :] = jnp.where(place < SPACE - 1, coupling[32:40, :], 0.0)

    film_lane = lax.broadcasted_iota(jnp.int32, (8, GRID), 1)
    for g in range(4):
        top = 8 + 8 * g
        mid = coupling[top : top + 8, :]
        scaled = stiffness * mid
        up = scaled * coupling[top - 1 : top + 7, :]
        down = scaled * coupling[top + 1 : top + 9, :]
        left = jnp.where(film_lane == 0, 0.0, scaled * pltpu.roll(mid, 1, 1))
        right = jnp.where(film_lane == GRID - 1, 0.0, scaled * pltpu.roll(mid, GRID - 1, 1))
        rows = slice(8 * g, 8 * g + 8)
        weights[0, rows, :] = up
        weights[1, rows, :] = down
        weights[2, rows, :] = left
        weights[3, rows, :] = right
        weights[4, rows, :] = (up + down) + (left + right)

    def exchange(slot, g):
        top = 8 + 8 * g
        rows = slice(8 * g, 8 * g + 8)
        w = [weights[k, rows, :] for k in range(5)]
        magnet, result = [], []
        for c in range(3):
            mid = state[slot, c, top : top + 8, :]
            total = w[0] * state[slot, c, top - 1 : top + 7, :]
            total = total + w[1] * state[slot, c, top + 1 : top + 9, :]
            total = total + w[2] * pltpu.roll(mid, 1, 1)
            total = total + w[3] * pltpu.roll(mid, GRID - 1, 1)
            magnet.append(mid)
            result.append(total - w[4] * mid)
        return magnet, result

    def coarse_group(slot, g):
        magnet, effective = exchange(slot, g)
        rows = slice(8 * g, 8 * g + 8)
        effective = [effective[c] + field[c, rows, :] for c in range(3)]
        effective[2] = effective[2] - magnet[2]
        rate = torque(magnet, effective)
        return [magnet[c] + (FINE * step_time) * rate[c] for c in range(3)]

    def source_slot(n):
        return jnp.where(n == 0, 2, n % 2)

    def first_sweep(n, carry):
        for g in range(4):
            new = coarse_group(source_slot(n), g)
            for c in range(3):
                state[(n + 1) % 2, c, 8 + 8 * g : 16 + 8 * g, :] = new[c]
        return carry

    lax.fori_loop(0, slice_index, first_sweep, 0)
    start_slot = source_slot(slice_index)
    for g in (1, 2):
        new = coarse_group(start_slot, g)
        for c in range(3):
            coarse_end[c, 8 * g - 8 : 8 * g, :] = new[c]
    for c in range(3):
        start = state[start_slot, c, 16:32, :]
        base[c, :, :] = start
        slope[c, :, :] = jnp.zeros_like(start)
        state[0, c, 16:32, :] = start

    low_half = lax.broadcasted_iota(jnp.int32, (ROWS, 128), 1) < 64
    even_quarter = (lax.broadcasted_iota(jnp.int32, (128, 128), 1) // 32) % 2 == 0

    def partner(value):
        return jnp.where(even_quarter, pltpu.roll(value, 32, 1), pltpu.roll(value, 96, 1))

    def send_column(worker, target):
        return pltpu.make_async_remote_copy(
            src_ref=outgoing.at[worker],
            dst_ref=columns.at[pl.ds(pl.multiple_of(ROWS * place, ROWS), ROWS), :],
            send_sem=out_send, recv_sem=out_recv,
            device_id=device(slice_index, target), device_id_type=MESH,
        )

    def send_back(target):
        return pltpu.make_async_remote_copy(
            src_ref=answer.at[pl.ds(pl.multiple_of(ROWS * target, ROWS), ROWS), :],
            dst_ref=returned.at[rank],
            send_sem=back_send, recv_sem=back_recv,
            device_id=device(slice_index, target), device_id_type=MESH,
        )

    def wait_bytes(ref, semaphore):
        pltpu.make_async_copy(ref, ref, semaphore).wait()

    def evaluation(e, carry):
        slot = e % 2
        for c in range(3):
            edges[c : c + 1, :] = state[0, c, 16:17, :]
            edges[3 + c : 4 + c, :] = state[0, c, 31:32, :]
        edge_copies = [
            pltpu.make_async_remote_copy(
                src_ref=edges, dst_ref=edge_in.at[slot, side],
                send_sem=edge_send.at[side], recv_sem=edge_recv.at[slot, side],
                device_id=device(slice_index, target), device_id_type=MESH,
            )
            for side, target in ((0, below), (1, above))
        ]
        for copy in edge_copies:
            copy.start()

        magnet = jnp.concatenate([state[0, c, 16:32, :] for c in range(3)], axis=0)
        high, low = split(magnet)
        stacked = jnp.concatenate([high, low], axis=0)
        for part in range(4):
            cols = slice(256 * part, 256 * part + 256)
            wide = dot(stacked, e1_high[:, cols])
            spectrum = wide[0:48] + wide[48:96] + dot(high, e1_low[:, cols])
            for half in range(2):
                t = 2 * part + half
                lanes = slice(128 * half, 128 * half + 128)
                mx, my, mz = spectrum[0:16, lanes], spectrum[16:32, lanes], spectrum[32:48, lanes]
                outgoing[2 * t] = jnp.where(low_half, mx, pltpu.roll(my, 64, 1))
                outgoing[2 * t + 1] = jnp.where(low_half, pltpu.roll(mx, 64, 1), my)
                outgoing[PAIRED + t] = mz

        for dz, dy in send_order():

            @pl.when((offset + dy - dz) % 4 != 3)
            def _(dz=dz, dy=dy):
                send_column(3 * ((place_z + dz) % 8) + (offset + dy - dz) % 4, at(dz, dy)).start()

        @pl.when(works)
        def _():
            columns[pl.ds(pl.multiple_of(ROWS * place, ROWS), ROWS), :] = outgoing[rank]

        for copy in edge_copies:
            copy.wait()
        for c in range(3):
            state[0, c, 15:16, :] = edge_in[slot, 0, 3 + c : 4 + c, :]
            state[0, c, 32:33, :] = edge_in[slot, 1, c : c + 1, :]
        for g in (1, 2):
            _, effective = exchange(0, g)
            for c in range(3):
                local_field[c, 8 * g - 8 : 8 * g, :] = effective[c] + field[c, 8 * g : 8 * g + 8, :]

        @pl.when(works)
        def _():
            wait_bytes(columns.at[pl.ds(0, ROWS * (SPACE - 1)), :], out_recv)
            column_high, column_low = split(columns[...])
            column_both = jnp.concatenate([column_high, column_low], axis=1)
            for part in range(4):
                rows = slice(256 * part, 256 * part + 256)
                wide = dot(e2_high[rows, :], column_both)
                spectrum = wide[:, 0:128] + wide[:, 128:256] + dot(e2_low[rows, :], column_high)
                spectrum = spectrum.reshape(4, 2, 32, 128)
                real = spectrum[:, 0].reshape(128, 128)
                imag = spectrum[:, 1].reshape(128, 128)
                diag = diagonal[rows, :].reshape(4, 2, 32, 128)
                mix = cross_term[128 * part : 128 * part + 128, :]
                real_out = diag[:, 0].reshape(128, 128) * real + mix * partner(imag)
                imag_out = diag[:, 1].reshape(128, 128) * imag - mix * partner(real)
                both = jnp.stack(
                    [real_out.reshape(4, 32, 128), imag_out.reshape(4, 32, 128)], axis=1
                ).reshape(256, 128)
                both_high, both_low = split(both)
                mixed[rows, 0:128] = both_high
                mixed[rows, 128:256] = both_low
            for parts in ((2,), (1, 3), (0,)):
                for k in parts:
                    rows = pl.ds(pl.multiple_of(128 * ((place_z // 2 + k) % 4), 128), 128)
                    wide = dot(e1_high[rows, :], mixed[...])
                    answer[rows, :] = wide[:, 0:128] + wide[:, 128:256] + dot(e1_low[rows, :], mixed[:, 0:128])
                planes = [(k, 1 if k == 1 else 0) for k in parts] + [(k, 0 if k == 1 else 1) for k in parts]
                for dy in (2, 1, -1, 0):
                    for k, half in planes:
                        target = 4 * (2 * ((place_z // 2 + k) % 4) + half) + (place_y + dy) % 4
                        if k == 0 and dy == 0:

                            @pl.when(target != place)
                            def _(target=target):
                                send_back(target).start()

                        else:
                            send_back(target).start()

            returned[rank] = answer[pl.ds(pl.multiple_of(ROWS * place, ROWS), ROWS), :]
            wait_bytes(outgoing.at[pl.ds(0, WORKERS - 1)], out_send)
            wait_bytes(returned.at[pl.ds(0, WORKERS - 1)], back_recv)

        @pl.when(jnp.logical_not(works))
        def _():
            wait_bytes(outgoing, out_send)
            wait_bytes(returned, back_recv)

        parts = [[], [], []]
        for t in range(8):
            first, second = returned[2 * t], returned[2 * t + 1]
            parts[0].append(jnp.where(low_half, first, pltpu.roll(second, 64, 1)))
            parts[1].append(jnp.where(low_half, pltpu.roll(first, 64, 1), second))
            parts[2].append(returned[PAIRED + t])
        spectrum = jnp.concatenate([jnp.concatenate(part, axis=1) for part in parts], axis=0)
        spectrum_high, spectrum_low = split(spectrum)
        wide = dot(jnp.concatenate([spectrum_high, spectrum_low], axis=0), e2_high[...])
        demag = wide[0:48] + wide[48:96] + dot(spectrum_high, e2_low[...])

        corrects = slot == 1
        length = jnp.where(corrects, 0.5 * step_time, step_time)
        for g in range(2):
            rows = slice(8 * g, 8 * g + 8)
            here = [state[0, c, 16 + 8 * g : 24 + 8 * g, :] for c in range(3)]
            effective = [local_field[c, rows, :] + demag[16 * c + 8 * g : 16 * c + 8 * g + 8] for c in range(3)]
            rate = torque(here, effective)
            for c in range(3):
                start = base[c, rows, :]
                new = start + length * (slope[c, rows, :] + rate[c])
                state[0, c, 16 + 8 * g : 24 + 8 * g, :] = new
                slope[c, rows, :] = jnp.where(corrects, 0.0, rate[c])
                base[c, rows, :] = jnp.where(corrects, new, start)

        @pl.when(works)
        def _():
            wait_bytes(answer.at[pl.ds(0, ROWS * (SPACE - 1)), :], back_send)

        return carry

    lax.fori_loop(0, 2 * FINE, evaluation, 0)

    for c in range(3):
        jumps[slice_index, c, 8:24, :] = state[0, c, 16:32, :] - coarse_end[c, :, :]
    jump_halo = [
        pltpu.make_async_remote_copy(
            src_ref=jumps.at[slice_index, :, pl.ds(source_row, 8), :],
            dst_ref=jumps.at[slice_index, :, pl.ds(landing_row, 8), :],
            send_sem=jump_send.at[side], recv_sem=jump_recv.at[side],
            device_id=device(slice_index, target), device_id_type=MESH,
        )
        for side, target, source_row, landing_row in ((0, below, 16, 0), (1, above, 8, 24))
    ]
    for copy in jump_halo:
        copy.start()
    for copy in jump_halo:
        copy.wait()

    def send_jump(n, target, semaphore):
        return pltpu.make_async_remote_copy(
            src_ref=jumps.at[n], dst_ref=jumps.at[n],
            send_sem=semaphore, recv_sem=gather_recv.at[n],
            device_id=device(target, place), device_id_type=MESH,
        )

    mate = slice_index + 1 - 2 * core

    @pl.when(core == 0)
    def _():
        send_jump(slice_index, mate, gather_send.at[0]).start()

    for i in (1, 2, 3):

        @pl.when(chip + i < TM // 2)
        def _(i=i):
            send_jump(slice_index, slice_index + 2 * i, gather_send.at[i]).start()

    def second_sweep(n, carry):
        @pl.when(n < slice_index)
        def _():
            wait_bytes(jumps.at[n], gather_recv.at[n])

        @pl.when((n < slice_index) & (n % 2 == core))
        def _():
            send_jump(n, mate, forward_send.at[n]).start()

        for g in range(4):
            new = coarse_group(source_slot(n), g)
            for c in range(3):
                state[(n + 1) % 2, c, 8 + 8 * g : 16 + 8 * g, :] = new[c] + jumps[n, c, 8 * g : 8 * g + 8, :]
        return carry

    lax.fori_loop(0, slice_index + 1, second_sweep, 0)
    for c in range(3):
        out[c] = state[(slice_index + 1) % 2, c, 16:32, :]

    def finish_forward(n, carry):
        @pl.when(n % 2 == core)
        def _():
            wait_bytes(jumps.at[n], forward_send.at[n])

        return carry

    lax.fori_loop(0, slice_index, finish_forward, 0)

    @pl.when(core == 0)
    def _():
        wait_bytes(jumps.at[slice_index], gather_send.at[0])

    for i in (1, 2, 3):

        @pl.when(chip + i < TM // 2)
        def _(i=i):
            wait_bytes(jumps.at[slice_index], gather_send.at[i])


def solution(mesh):
    tables = twiddle_tables()
    vmem = pltpu.VMEM
    dma = pltpu.SemaphoreType.DMA
    scratch = [
        vmem((3, 3, 48, GRID), F32),
        vmem((3, 32, GRID), F32),
        vmem((48, GRID), F32),
        vmem((5, 32, GRID), F32),
        vmem((GRID, LENGTH), BF16),
        vmem((GRID, LENGTH), BF16),
        vmem((LENGTH, GRID), BF16),
        vmem((LENGTH, GRID), BF16),
        vmem((LENGTH, 128), F32),
        vmem((GRID, 128), F32),
        vmem((WORKERS, ROWS, 128), F32),
        vmem((GRID, 128), F32),
        vmem((LENGTH, 256), BF16),
        vmem((GRID, 128), F32),
        vmem((WORKERS, ROWS, 128), F32),
        vmem((8, GRID), F32),
        vmem((2, 2, 8, GRID), F32),
        vmem((3, ROWS, GRID), F32),
        vmem((3, ROWS, GRID), F32),
        vmem((3, ROWS, GRID), F32),
        vmem((3, ROWS, GRID), F32),
        vmem((TM, 3, 32, GRID), F32),
        dma((2, 3)),
        dma((2, 3)),
        dma((2,)),
        dma((2, 2)),
        dma,
        dma,
        dma,
        dma,
        dma((2,)),
        dma((2,)),
        dma((4,)),
        dma((TM,)),
        dma((TM,)),
    ]

    def shards(initial_state, applied_field, coupling):
        by_component = [jnp.transpose(value, (1, 0, 2)) for value in (initial_state, applied_field)]
        result = pl.pallas_call(
            kernel,
            out_shape=jax.ShapeDtypeStruct((3, ROWS, GRID), F32),
            in_specs=[pl.BlockSpec(memory_space=pltpu.VMEM)] * 7,
            out_specs=pl.BlockSpec(memory_space=pltpu.VMEM),
            scratch_shapes=scratch,
            compiler_params=pltpu.CompilerParams(collective_id=0, has_side_effects=True),
        )(*by_component, coupling, *[jnp.asarray(table) for table in tables])
        return jnp.transpose(result, (1, 0, 2))[None]

    return jax.shard_map(
        shards,
        mesh=mesh,
        in_specs=(P("space", None, None), P("space", None, None), P("space", None)),
        out_specs=P("tm", "space", None, None),
        check_vma=False,
    )
```

```python
import math

import jax
import jax.numpy as jnp
import numpy as np
from jax import lax
from jax.experimental import pallas as pl
from jax.experimental.pallas import tpu as pltpu
from jax.sharding import PartitionSpec as P

MESH = pl.DeviceIdType.MESH
F32 = jnp.float32
BF16 = jnp.bfloat16

FINE = 2
step_time = 0.06
damping = 0.02
stiffness = 0.25
thickness = 8.0

GRID = 512
LENGTH = 2 * GRID
ROWS = 16
SPACE = 32
TM = 8
WORKERS = 24
PAIRED = 16


def send_order():
    order = []
    for far in (4, 3, 2, 1, 0):
        for dy in (2, 1, -1, 0):
            for dz in (far, -far) if far in (1, 2, 3) else (far,):
                order.append((dz, dy if dz >= 0 else -dy))
    return [pair for pair in order if pair != (0, 0)]


def twiddle_tables():
    unit = 2.0 * np.pi / LENGTH
    col = np.arange(LENGTH)
    wave = 32 * (col // 64) + col % 32
    kind = (col // 32) % 2
    phase = np.where(kind == 1, np.pi / 2, 0.0)
    nyquist = (kind == 1) & (wave == 0)
    wave = np.where(nyquist, GRID, wave)
    phase = np.where(nyquist, 0.0, phase)
    coarse = 16 * np.arange(GRID // 16)[:, None]
    fine = np.arange(16)[:, None]
    angle_coarse = unit * (coarse * wave % LENGTH)
    angle_fine = unit * (fine * wave % LENGTH) + phase
    x = np.arange(GRID)[None, :]
    block = 32 * np.arange(GRID // 32)[:, None]
    inner = np.arange(64)[:, None]
    angle_block = unit * (block * x % LENGTH)
    angle_inner = unit * (inner % 32 * x % LENGTH) + np.where(inner >= 32, np.pi / 2, 0.0)

    def both(angle):
        return np.concatenate([np.cos(angle), np.sin(angle)], axis=0).astype(np.float32)

    return both(angle_coarse), both(angle_fine), both(angle_block), both(angle_inner)


def split(value):
    high = value.astype(BF16)
    return high, (value - high.astype(F32)).astype(BF16)


def dot(left, right):
    return jnp.dot(left, right, preferred_element_type=F32)


def cross(a, b):
    return [
        a[1] * b[2] - a[2] * b[1],
        a[2] * b[0] - a[0] * b[2],
        a[0] * b[1] - a[1] * b[0],
    ]


def torque(magnet, effective):
    first = cross(magnet, effective)
    second = cross(magnet, first)
    scale = -1.0 / (1.0 + damping * damping)
    return [scale * (f + damping * s) for f, s in zip(first, second)]


def kernel(
    state_in, field_in, coupling_in, t_coarse, t_fine, t_block, t_inner, out,
    state, field, coupling, weights, e1_high, e1_low, e2_high, e2_low, diagonal, cross_term,
    outgoing, columns, mixed, answer, returned, edges, edge_in, base, slope, local_field, coarse_end, jumps,
    halo_send, halo_recv, edge_send, edge_recv, out_send, out_recv, back_send, back_recv,
    gather_send, gather_recv, rim_send, rim_recv, forward_send, forward_recv,
):
    slice_index = lax.axis_index("tm")
    place = lax.axis_index("space")

    def device(which_slice, which_place):
        return (which_slice, which_place)

    chip = slice_index // 2
    core = slice_index % 2
    above = (place + SPACE - 1) % SPACE
    below = (place + 1) % SPACE
    offset = (place % 4 - (place // 4) % 4 + 3) % 4
    rank = 3 * (place // 4) + offset
    works = offset < 3
    rank = jnp.minimum(rank, WORKERS - 1)

    place_z, place_y = place // 4, place % 4

    def at(dz, dy):
        return 4 * ((place_z + dz) % 8) + (place_y + dy) % 4

    barrier = pltpu.get_barrier_semaphore()

    def greet_space(i, carry):
        pl.semaphore_signal(barrier, inc=1, device_id=device(slice_index, (place + i) % SPACE), device_id_type=MESH)
        return carry

    def greet_tm(i, carry):
        pl.semaphore_signal(barrier, inc=1, device_id=device((slice_index + i) % TM, place), device_id_type=MESH)
        return carry

    lax.fori_loop(1, SPACE, greet_space, 0)
    lax.fori_loop(1, TM, greet_tm, 0)

    zero_rows = jnp.zeros((8, GRID), F32)
    for c in range(3):
        for slot in range(3):
            state[slot, c, 0:8, :] = zero_rows
            state[slot, c, 40:48, :] = zero_rows
        state[2, c, 16:32, :] = state_in[c]
        field[c, 8:24, :] = field_in[c]
    coupling[0:8, :] = zero_rows
    coupling[40:48, :] = zero_rows
    coupling[16:32, :] = coupling_in[...]
    edges[...] = zero_rows

    pl.semaphore_wait(barrier, SPACE - 1 + TM - 1)

    def halo_copies():
        copies = []
        for side, target, source_row, landing_row in ((0, below, 24, 8), (1, above, 16, 32)):
            for what, (source, landing) in enumerate(
                (
                    (state.at[2, :, pl.ds(source_row, 8), :], state.at[2, :, pl.ds(landing_row, 8), :]),
                    (field.at[:, pl.ds(source_row - 8, 8), :], field.at[:, pl.ds(landing_row - 8, 8), :]),
                    (coupling.at[pl.ds(source_row, 8), :], coupling.at[pl.ds(landing_row, 8), :]),
                )
            ):
                copies.append(
                    pltpu.make_async_remote_copy(
                        src_ref=source, dst_ref=landing,
                        send_sem=halo_send.at[side, what], recv_sem=halo_recv.at[side, what],
                        device_id=device(slice_index, target), device_id_type=MESH,
                    )
                )
        return copies

    first_halo = halo_copies()
    for copy in first_halo:
        copy.start()

    def build_e1(a, carry):
        value = t_coarse[pl.ds(a, 1), :] * t_fine[0:16, :] - t_coarse[pl.ds(32 + a, 1), :] * t_fine[16:32, :]
        high, low = split(value)
        rows = pl.ds(pl.multiple_of(16 * a, 16), 16)
        e1_high[rows, :] = high
        e1_low[rows, :] = low
        return carry

    lax.fori_loop(0, GRID // 16, build_e1, 0)
    inner_row = lax.broadcasted_iota(jnp.int32, (64, GRID), 0)
    inner_lane = lax.broadcasted_iota(jnp.int32, (64, GRID), 1)
    alternating = (1 - 2 * (inner_lane % 2)).astype(F32)

    def build_e2(j, carry):
        value = t_block[pl.ds(j, 1), :] * t_inner[0:64, :] - t_block[pl.ds(16 + j, 1), :] * t_inner[64:128, :]
        value = jnp.where((inner_row == 32) & (j == 0), alternating, value)
        high, low = split(value)
        rows = pl.ds(pl.multiple_of(64 * j, 64), 64)
        e2_high[rows, :] = high
        e2_low[rows, :] = low
        return carry

    lax.fori_loop(0, GRID // 32, build_e2, 0)

    def build_tensor(chunk, carry):
        row = 256 * chunk + lax.broadcasted_iota(jnp.int32, (256, 128), 0)
        lane = lax.broadcasted_iota(jnp.int32, (256, 128), 1)
        quarter = lane // 32
        paired = rank < PAIRED
        wave_y = 32 * (row // 64) + row % 32
        wave_y = jnp.where((wave_y == 0) & ((row // 32) % 2 == 1), GRID, wave_y)
        first_x = jnp.where(paired, 32 * rank, 64 * (rank - PAIRED) + 32 * (quarter // 2))
        wave_x = first_x + lane % 32
        wave_x = jnp.where((wave_x == 0) & (quarter % 2 == 1), GRID, wave_x)
        edge_x = (wave_x == 0) | (wave_x == GRID)
        edge_y = (wave_y == 0) | (wave_y == GRID)
        factor = jnp.where(edge_x, 1.0, 2.0) * jnp.where(edge_y, 1.0, 2.0) * (-1.0 / (LENGTH * LENGTH))
        q_x = wave_x.astype(F32) * (2.0 * math.pi / LENGTH)
        q_y = wave_y.astype(F32) * (2.0 * math.pi / LENGTH)
        squared = q_x * q_x + q_y * q_y
        nonzero = (wave_x + wave_y) > 0
        safe = jnp.where(nonzero, squared, 1.0)
        scaled = jnp.sqrt(safe) * thickness
        film = jnp.where(nonzero, (1.0 - jnp.exp(-scaled)) / scaled, 1.0)
        in_plane = (1.0 - film) / safe
        own_wave = jnp.where(quarter < 2, q_x, q_y)
        diag = jnp.where(paired, in_plane * own_wave * own_wave, film)
        sign = jnp.where(quarter % 2 == 0, -1.0, 1.0)
        mix = jnp.where(edge_x | edge_y | jnp.logical_not(paired), 0.0, sign * in_plane * q_x * q_y)
        diagonal[pl.ds(pl.multiple_of(256 * chunk, 256), 256), :] = diag * factor
        mix = (mix * factor).reshape(4, 2, 32, 128)[:, 0].reshape(128, 128)
        cross_term[pl.ds(pl.multiple_of(128 * chunk, 128), 128), :] = mix
        return carry

    lax.fori_loop(0, 4, build_tensor, 0)

    for copy in first_halo:
        copy.wait()
    coupling[8:16, :] = jnp.where(place > 0, coupling[8:16, :], 0.0)
    coupling[32:40, :] = jnp.where(place < SPACE - 1, coupling[32:40, :], 0.0)

    film_lane = lax.broadcasted_iota(jnp.int32, (8, GRID), 1)
    for g in range(4):
        top = 8 + 8 * g
        mid = coupling[top : top + 8, :]
        scaled = stiffness * mid
        up = scaled * coupling[top - 1 : top + 7, :]
        down = scaled * coupling[top + 1 : top + 9, :]
        left = jnp.where(film_lane == 0, 0.0, scaled * pltpu.roll(mid, 1, 1))
        right = jnp.where(film_lane == GRID - 1, 0.0, scaled * pltpu.roll(mid, GRID - 1, 1))
        rows = slice(8 * g, 8 * g + 8)
        weights[0, rows, :] = up
        weights[1, rows, :] = down
        weights[2, rows, :] = left
        weights[3, rows, :] = right
        weights[4, rows, :] = (up + down) + (left + right)

    def exchange(slot, g):
        top = 8 + 8 * g
        rows = slice(8 * g, 8 * g + 8)
        w = [weights[k, rows, :] for k in range(5)]
        magnet, result = [], []
        for c in range(3):
            mid = state[slot, c, top : top + 8, :]
            total = w[0] * state[slot, c, top - 1 : top + 7, :]
            total = total + w[1] * state[slot, c, top + 1 : top + 9, :]
            total = total + w[2] * pltpu.roll(mid, 1, 1)
            total = total + w[3] * pltpu.roll(mid, GRID - 1, 1)
            magnet.append(mid)
            result.append(total - w[4] * mid)
        return magnet, result

    def coarse_group(slot, g):
        magnet, effective = exchange(slot, g)
        rows = slice(8 * g, 8 * g + 8)
        effective = [effective[c] + field[c, rows, :] for c in range(3)]
        effective[2] = effective[2] - magnet[2]
        rate = torque(magnet, effective)
        return [magnet[c] + (FINE * step_time) * rate[c] for c in range(3)]

    def source_slot(n):
        return jnp.where(n == 0, 2, n % 2)

    def first_sweep(n, carry):
        for g in range(4):
            new = coarse_group(source_slot(n), g)
            for c in range(3):
                state[(n + 1) % 2, c, 8 + 8 * g : 16 + 8 * g, :] = new[c]
        return carry

    lax.fori_loop(0, slice_index, first_sweep, 0)
    start_slot = source_slot(slice_index)
    for g in (1, 2):
        new = coarse_group(start_slot, g)
        for c in range(3):
            coarse_end[c, 8 * g - 8 : 8 * g, :] = new[c]
    for c in range(3):
        start = state[start_slot, c, 16:32, :]
        base[c, :, :] = start
        slope[c, :, :] = jnp.zeros_like(start)
        state[0, c, 16:32, :] = start

    low_half = lax.broadcasted_iota(jnp.int32, (ROWS, 128), 1) < 64
    even_quarter = (lax.broadcasted_iota(jnp.int32, (128, 128), 1) // 32) % 2 == 0

    def partner(value):
        return jnp.where(even_quarter, pltpu.roll(value, 32, 1), pltpu.roll(value, 96, 1))

    def send_column(worker, target):
        return pltpu.make_async_remote_copy(
            src_ref=outgoing.at[worker],
            dst_ref=columns.at[pl.ds(pl.multiple_of(ROWS * place, ROWS), ROWS), :],
            send_sem=out_send, recv_sem=out_recv,
            device_id=device(slice_index, target), device_id_type=MESH,
        )

    def send_back(target):
        return pltpu.make_async_remote_copy(
            src_ref=answer.at[pl.ds(pl.multiple_of(ROWS * target, ROWS), ROWS), :],
            dst_ref=returned.at[rank],
            send_sem=back_send, recv_sem=back_recv,
            device_id=device(slice_index, target), device_id_type=MESH,
        )

    def wait_bytes(ref, semaphore):
        pltpu.make_async_copy(ref, ref, semaphore).wait()

    def evaluation(e, carry):
        slot = e % 2
        for c in range(3):
            edges[c : c + 1, :] = state[0, c, 16:17, :]
            edges[3 + c : 4 + c, :] = state[0, c, 31:32, :]
        edge_copies = [
            pltpu.make_async_remote_copy(
                src_ref=edges, dst_ref=edge_in.at[slot, side],
                send_sem=edge_send.at[side], recv_sem=edge_recv.at[slot, side],
                device_id=device(slice_index, target), device_id_type=MESH,
            )
            for side, target in ((0, below), (1, above))
        ]
        for copy in edge_copies:
            copy.start()

        magnet = jnp.concatenate([state[0, c, 16:32, :] for c in range(3)], axis=0)
        high, low = split(magnet)
        stacked = jnp.concatenate([high, low], axis=0)
        for part in range(4):
            cols = slice(256 * part, 256 * part + 256)
            wide = dot(stacked, e1_high[:, cols])
            spectrum = wide[0:48] + wide[48:96] + dot(high, e1_low[:, cols])
            for half in range(2):
                t = 2 * part + half
                lanes = slice(128 * half, 128 * half + 128)
                mx, my, mz = spectrum[0:16, lanes], spectrum[16:32, lanes], spectrum[32:48, lanes]
                outgoing[2 * t] = jnp.where(low_half, mx, pltpu.roll(my, 64, 1))
                outgoing[2 * t + 1] = jnp.where(low_half, pltpu.roll(mx, 64, 1), my)
                outgoing[PAIRED + t] = mz

        for dz, dy in send_order():

            @pl.when((offset + dy - dz) % 4 != 3)
            def _(dz=dz, dy=dy):
                send_column(3 * ((place_z + dz) % 8) + (offset + dy - dz) % 4, at(dz, dy)).start()

        @pl.when(works)
        def _():
            columns[pl.ds(pl.multiple_of(ROWS * place, ROWS), ROWS), :] = outgoing[rank]

        for copy in edge_copies:
            copy.wait()
        for c in range(3):
            state[0, c, 15:16, :] = edge_in[slot, 0, 3 + c : 4 + c, :]
            state[0, c, 32:33, :] = edge_in[slot, 1, c : c + 1, :]
        for g in (1, 2):
            _, effective = exchange(0, g)
            for c in range(3):
                local_field[c, 8 * g - 8 : 8 * g, :] = effective[c] + field[c, 8 * g : 8 * g + 8, :]

        @pl.when(works)
        def _():
            wait_bytes(columns.at[pl.ds(0, ROWS * (SPACE - 1)), :], out_recv)
            column_high, column_low = split(columns[...])
            column_both = jnp.concatenate([column_high, column_low], axis=1)
            for part in range(4):
                rows = slice(256 * part, 256 * part + 256)
                wide = dot(e2_high[rows, :], column_both)
                spectrum = wide[:, 0:128] + wide[:, 128:256] + dot(e2_low[rows, :], column_high)
                spectrum = spectrum.reshape(4, 2, 32, 128)
                real = spectrum[:, 0].reshape(128, 128)
                imag = spectrum[:, 1].reshape(128, 128)
                diag = diagonal[rows, :].reshape(4, 2, 32, 128)
                mix = cross_term[128 * part : 128 * part + 128, :]
                real_out = diag[:, 0].reshape(128, 128) * real + mix * partner(imag)
                imag_out = diag[:, 1].reshape(128, 128) * imag - mix * partner(real)
                both = jnp.stack(
                    [real_out.reshape(4, 32, 128), imag_out.reshape(4, 32, 128)], axis=1
                ).reshape(256, 128)
                both_high, both_low = split(both)
                mixed[rows, 0:128] = both_high
                mixed[rows, 128:256] = both_low
            for parts in ((2,), (1, 3), (0,)):
                for k in parts:
                    rows = pl.ds(pl.multiple_of(128 * ((place_z // 2 + k) % 4), 128), 128)
                    wide = dot(e1_high[rows, :], mixed[...])
                    answer[rows, :] = wide[:, 0:128] + wide[:, 128:256] + dot(e1_low[rows, :], mixed[:, 0:128])
                planes = [(k, 1 if k == 1 else 0) for k in parts] + [(k, 0 if k == 1 else 1) for k in parts]
                for dy in (2, 1, -1, 0):
                    for k, half in planes:
                        target = 4 * (2 * ((place_z // 2 + k) % 4) + half) + (place_y + dy) % 4
                        if k == 0 and dy == 0:

                            @pl.when(target != place)
                            def _(target=target):
                                send_back(target).start()

                        else:
                            send_back(target).start()

            returned[rank] = answer[pl.ds(pl.multiple_of(ROWS * place, ROWS), ROWS), :]
            wait_bytes(outgoing.at[pl.ds(0, WORKERS - 1)], out_send)
            wait_bytes(returned.at[pl.ds(0, WORKERS - 1)], back_recv)

        @pl.when(jnp.logical_not(works))
        def _():
            wait_bytes(outgoing, out_send)
            wait_bytes(returned, back_recv)

        parts = [[], [], []]
        for t in range(8):
            first, second = returned[2 * t], returned[2 * t + 1]
            parts[0].append(jnp.where(low_half, first, pltpu.roll(second, 64, 1)))
            parts[1].append(jnp.where(low_half, pltpu.roll(first, 64, 1), second))
            parts[2].append(returned[PAIRED + t])
        spectrum = jnp.concatenate([jnp.concatenate(part, axis=1) for part in parts], axis=0)
        spectrum_high, spectrum_low = split(spectrum)
        wide = dot(jnp.concatenate([spectrum_high, spectrum_low], axis=0), e2_high[...])
        demag = wide[0:48] + wide[48:96] + dot(spectrum_high, e2_low[...])

        corrects = slot == 1
        length = jnp.where(corrects, 0.5 * step_time, step_time)
        for g in range(2):
            rows = slice(8 * g, 8 * g + 8)
            here = [state[0, c, 16 + 8 * g : 24 + 8 * g, :] for c in range(3)]
            effective = [local_field[c, rows, :] + demag[16 * c + 8 * g : 16 * c + 8 * g + 8] for c in range(3)]
            rate = torque(here, effective)
            for c in range(3):
                start = base[c, rows, :]
                new = start + length * (slope[c, rows, :] + rate[c])
                state[0, c, 16 + 8 * g : 24 + 8 * g, :] = new
                slope[c, rows, :] = jnp.where(corrects, 0.0, rate[c])
                base[c, rows, :] = jnp.where(corrects, new, start)

        @pl.when(works)
        def _():
            wait_bytes(answer.at[pl.ds(0, ROWS * (SPACE - 1)), :], back_send)

        return carry

    lax.fori_loop(0, 2 * FINE, evaluation, 0)

    own = slice_index
    mate = own + 1 - 2 * core
    for c in range(3):
        jumps[own, c, 8:24, :] = state[0, c, 16:32, :] - coarse_end[c, :, :]

    def send_rows(i):
        return pltpu.make_async_remote_copy(
            src_ref=jumps.at[own, :, pl.ds(8, ROWS), :], dst_ref=jumps.at[own, :, pl.ds(8, ROWS), :],
            send_sem=gather_send.at[i], recv_sem=gather_recv.at[own],
            device_id=device(own + 2 * i, place), device_id_type=MESH,
        )

    def send_rims(n):
        return [
            pltpu.make_async_remote_copy(
                src_ref=jumps.at[n, :, pl.ds(source_row, 8), :], dst_ref=jumps.at[n, :, pl.ds(landing_row, 8), :],
                send_sem=rim_send.at[n, side], recv_sem=rim_recv.at[n, side],
                device_id=device(slice_index, target), device_id_type=MESH,
            )
            for side, target, source_row, landing_row in ((0, below, 16, 0), (1, above, 8, 24))
        ]

    def send_mate(n):
        return pltpu.make_async_remote_copy(
            src_ref=jumps.at[n], dst_ref=jumps.at[n],
            send_sem=forward_send.at[n], recv_sem=forward_recv.at[n],
            device_id=device(mate, place), device_id_type=MESH,
        )

    def holds(i):
        return core == 0 if i == 0 else chip >= i

    def start_rims(i):
        @pl.when(holds(i))
        def _():
            if i > 0:
                wait_bytes(jumps.at[own - 2 * i, :, pl.ds(8, ROWS), :], gather_recv.at[own - 2 * i])
            for copy in send_rims(own - 2 * i):
                copy.start()

    def pass_on(i):
        @pl.when(holds(i))
        def _():
            for copy in send_rims(own - 2 * i):
                copy.wait_recv()
            send_mate(own - 2 * i).start()

    start_rims(0)
    for i in (2, 3, 1):

        @pl.when(chip + i < TM // 2)
        def _(i=i):
            send_rows(i).start()

    start_rims(1)
    start_rims(3)
    start_rims(2)
    pass_on(0)
    pass_on(1)
    pass_on(3)

    def second_sweep(n, carry):
        @pl.when((chip >= 2) & (n == 2 * chip - 4))
        def _():
            pass_on(2)

        @pl.when(n % 2 != core)
        def _():
            wait_bytes(jumps.at[n], forward_recv.at[n])

        for g in range(4):
            new = coarse_group(source_slot(n), g)
            for c in range(3):
                state[(n + 1) % 2, c, 8 + 8 * g : 16 + 8 * g, :] = new[c] + jumps[n, c, 8 * g : 8 * g + 8, :]
        return carry

    lax.fori_loop(0, own, second_sweep, 0)
    for g in (1, 2):
        new = coarse_group(source_slot(own), g)
        for c in range(3):
            out[c, 8 * g - 8 : 8 * g, :] = new[c] + jumps[own, c, 8 * g : 8 * g + 8, :]

    for i in range(4):

        @pl.when(holds(i))
        def _(i=i):
            for copy in send_rims(own - 2 * i):
                copy.wait_send()
            send_mate(own - 2 * i).wait_send()

        if i > 0:

            @pl.when(chip + i < TM // 2)
            def _(i=i):
                send_rows(i).wait_send()


def solution(mesh):
    tables = twiddle_tables()
    vmem = pltpu.VMEM
    dma = pltpu.SemaphoreType.DMA
    scratch = [
        vmem((3, 3, 48, GRID), F32),
        vmem((3, 32, GRID), F32),
        vmem((48, GRID), F32),
        vmem((5, 32, GRID), F32),
        vmem((GRID, LENGTH), BF16),
        vmem((GRID, LENGTH), BF16),
        vmem((LENGTH, GRID), BF16),
        vmem((LENGTH, GRID), BF16),
        vmem((LENGTH, 128), F32),
        vmem((GRID, 128), F32),
        vmem((WORKERS, ROWS, 128), F32),
        vmem((GRID, 128), F32),
        vmem((LENGTH, 256), BF16),
        vmem((GRID, 128), F32),
        vmem((WORKERS, ROWS, 128), F32),
        vmem((8, GRID), F32),
        vmem((2, 2, 8, GRID), F32),
        vmem((3, ROWS, GRID), F32),
        vmem((3, ROWS, GRID), F32),
        vmem((3, ROWS, GRID), F32),
        vmem((3, ROWS, GRID), F32),
        vmem((TM, 3, 32, GRID), F32),
        dma((2, 3)),
        dma((2, 3)),
        dma((2,)),
        dma((2, 2)),
        dma,
        dma,
        dma,
        dma,
        dma((4,)),
        dma((TM,)),
        dma((TM, 2)),
        dma((TM, 2)),
        dma((TM,)),
        dma((TM,)),
    ]

    def shards(initial_state, applied_field, coupling):
        by_component = [jnp.transpose(value, (1, 0, 2)) for value in (initial_state, applied_field)]
        result = pl.pallas_call(
            kernel,
            out_shape=jax.ShapeDtypeStruct((3, ROWS, GRID), F32),
            in_specs=[pl.BlockSpec(memory_space=pltpu.VMEM)] * 7,
            out_specs=pl.BlockSpec(memory_space=pltpu.VMEM),
            scratch_shapes=scratch,
            compiler_params=pltpu.CompilerParams(collective_id=0, has_side_effects=True),
        )(*by_component, coupling, *[jnp.asarray(table) for table in tables])
        return jnp.transpose(result, (1, 0, 2))[None]

    return jax.shard_map(
        shards,
        mesh=mesh,
        in_specs=(P("space", None, None), P("space", None, None), P("space", None)),
        out_specs=P("tm", "space", None, None),
        check_vma=False,
    )
```

```python
import math

import jax
import jax.numpy as jnp
import numpy as np
from jax import lax
from jax.experimental import pallas as pl
from jax.experimental.pallas import tpu as pltpu
from jax.sharding import PartitionSpec as P

MESH = pl.DeviceIdType.MESH
F32 = jnp.float32
BF16 = jnp.bfloat16

FINE = 2
step_time = 0.06
damping = 0.02
stiffness = 0.25
thickness = 8.0

GRID = 512
LENGTH = 2 * GRID
ROWS = 16
SPACE = 32
TM = 8
WORKERS = 24
PAIRED = 16


def twiddle_tables():
    unit = 2.0 * np.pi / LENGTH
    col = np.arange(LENGTH)
    wave = 32 * (col // 64) + col % 32
    kind = (col // 32) % 2
    phase = np.where(kind == 1, np.pi / 2, 0.0)
    nyquist = (kind == 1) & (wave == 0)
    wave = np.where(nyquist, GRID, wave)
    phase = np.where(nyquist, 0.0, phase)
    coarse = 16 * np.arange(GRID // 16)[:, None]
    fine = np.arange(16)[:, None]
    angle_coarse = unit * (coarse * wave % LENGTH)
    angle_fine = unit * (fine * wave % LENGTH) + phase
    x = np.arange(GRID)[None, :]
    block = 32 * np.arange(GRID // 32)[:, None]
    inner = np.arange(64)[:, None]
    angle_block = unit * (block * x % LENGTH)
    angle_inner = unit * (inner % 32 * x % LENGTH) + np.where(inner >= 32, np.pi / 2, 0.0)

    def both(angle):
        return np.concatenate([np.cos(angle), np.sin(angle)], axis=0).astype(np.float32)

    return both(angle_coarse), both(angle_fine), both(angle_block), both(angle_inner)


def split(value):
    high = value.astype(BF16)
    return high, (value - high.astype(F32)).astype(BF16)


def dot(left, right):
    return jnp.dot(left, right, preferred_element_type=F32)


def cross(a, b):
    return [
        a[1] * b[2] - a[2] * b[1],
        a[2] * b[0] - a[0] * b[2],
        a[0] * b[1] - a[1] * b[0],
    ]


def torque(magnet, effective):
    first = cross(magnet, effective)
    second = cross(magnet, first)
    scale = -1.0 / (1.0 + damping * damping)
    return [scale * (f + damping * s) for f, s in zip(first, second)]


def kernel(
    state_in, field_in, coupling_in, coarse_in, fine_in, block_in, inner_in, out,
    t_coarse, t_fine, t_block, t_inner, state, field, coupling, weights, e1_high, e1_low, e2_high, e2_low, diagonal, cross_term,
    outgoing, columns, mixed, answer, returned, edges, edge_in, base, slope, local_field, coarse_end, jumps,
    load, halo_send, halo_recv, edge_send, edge_recv, out_send, out_recv, back_send, back_recv,
    gather_send, gather_recv, rim_send, rim_recv, forward_send, forward_recv,
):
    slice_index = lax.axis_index("tm")
    place = lax.axis_index("space")

    def device(which_slice, which_place):
        return (which_slice, which_place)

    chip = slice_index // 2
    core = slice_index % 2
    above = (place + SPACE - 1) % SPACE
    below = (place + 1) % SPACE
    offset = (place % 4 - (place // 4) % 4 + 3) % 4
    works = offset < 3

    def number(plane, turn):
        return jnp.where(turn < 2, 2 * plane + turn, PAIRED + plane)

    rank = number(place // 4, jnp.minimum(offset, 2))

    place_z, place_y = place // 4, place % 4

    loads = [
        pltpu.make_async_copy(source, landing, load.at[i])
        for i, (source, landing) in enumerate(
            (
                (state_in, state.at[2, :, pl.ds(16, ROWS), :]),
                (field_in, field.at[:, pl.ds(8, ROWS), :]),
                (coupling_in, coupling.at[pl.ds(16, ROWS), :]),
                (coarse_in, t_coarse),
                (fine_in, t_fine),
                (block_in, t_block),
                (inner_in, t_inner),
            )
        )
    ]
    for copy in loads:
        copy.start()

    barrier = pltpu.get_barrier_semaphore()

    def greet_space(i, carry):
        pl.semaphore_signal(barrier, inc=1, device_id=device(slice_index, (place + i) % SPACE), device_id_type=MESH)
        return carry

    def greet_tm(i, carry):
        pl.semaphore_signal(barrier, inc=1, device_id=device((slice_index + i) % TM, place), device_id_type=MESH)
        return carry

    lax.fori_loop(1, SPACE, greet_space, 0)
    lax.fori_loop(1, TM, greet_tm, 0)

    zero_rows = jnp.zeros((8, GRID), F32)
    for c in range(3):
        for slot in range(3):
            state[slot, c, 0:8, :] = zero_rows
            state[slot, c, 40:48, :] = zero_rows
    coupling[0:8, :] = zero_rows
    coupling[40:48, :] = zero_rows
    edges[...] = zero_rows

    for copy in loads[:3]:
        copy.wait()
    pl.semaphore_wait(barrier, SPACE - 1 + TM - 1)

    def halo_copies():
        copies = []
        for side, target, source_row, landing_row in ((0, below, 24, 8), (1, above, 16, 32)):
            for what, (source, landing) in enumerate(
                (
                    (state.at[2, :, pl.ds(source_row, 8), :], state.at[2, :, pl.ds(landing_row, 8), :]),
                    (field.at[:, pl.ds(source_row - 8, 8), :], field.at[:, pl.ds(landing_row - 8, 8), :]),
                    (coupling.at[pl.ds(source_row, 8), :], coupling.at[pl.ds(landing_row, 8), :]),
                )
            ):
                copies.append(
                    pltpu.make_async_remote_copy(
                        src_ref=source, dst_ref=landing,
                        send_sem=halo_send.at[side, what], recv_sem=halo_recv.at[side, what],
                        device_id=device(slice_index, target), device_id_type=MESH,
                    )
                )
        return copies

    first_halo = halo_copies()
    for copy in first_halo:
        copy.start()

    for copy in loads[3:]:
        copy.wait()

    def build_e1(a, carry):
        value = t_coarse[pl.ds(a, 1), :] * t_fine[0:16, :] - t_coarse[pl.ds(32 + a, 1), :] * t_fine[16:32, :]
        high, low = split(value)
        rows = pl.ds(pl.multiple_of(16 * a, 16), 16)
        e1_high[rows, :] = high
        e1_low[rows, :] = low
        return carry

    lax.fori_loop(0, GRID // 16, build_e1, 0)
    inner_row = lax.broadcasted_iota(jnp.int32, (64, GRID), 0)
    inner_lane = lax.broadcasted_iota(jnp.int32, (64, GRID), 1)
    alternating = (1 - 2 * (inner_lane % 2)).astype(F32)

    def build_e2(j, carry):
        value = t_block[pl.ds(j, 1), :] * t_inner[0:64, :] - t_block[pl.ds(16 + j, 1), :] * t_inner[64:128, :]
        value = jnp.where((inner_row == 32) & (j == 0), alternating, value)
        high, low = split(value)
        rows = pl.ds(pl.multiple_of(64 * j, 64), 64)
        e2_high[rows, :] = high
        e2_low[rows, :] = low
        return carry

    lax.fori_loop(0, GRID // 32, build_e2, 0)

    def build_tensor(chunk, carry):
        row = 256 * chunk + lax.broadcasted_iota(jnp.int32, (256, 128), 0)
        lane = lax.broadcasted_iota(jnp.int32, (256, 128), 1)
        quarter = lane // 32
        paired = rank < PAIRED
        wave_y = 32 * (row // 64) + row % 32
        wave_y = jnp.where((wave_y == 0) & ((row // 32) % 2 == 1), GRID, wave_y)
        first_x = jnp.where(paired, 32 * rank, 64 * (rank - PAIRED) + 32 * (quarter // 2))
        wave_x = first_x + lane % 32
        wave_x = jnp.where((wave_x == 0) & (quarter % 2 == 1), GRID, wave_x)
        edge_x = (wave_x == 0) | (wave_x == GRID)
        edge_y = (wave_y == 0) | (wave_y == GRID)
        factor = jnp.where(edge_x, 1.0, 2.0) * jnp.where(edge_y, 1.0, 2.0) * (-1.0 / (LENGTH * LENGTH))
        q_x = wave_x.astype(F32) * (2.0 * math.pi / LENGTH)
        q_y = wave_y.astype(F32) * (2.0 * math.pi / LENGTH)
        squared = q_x * q_x + q_y * q_y
        nonzero = (wave_x + wave_y) > 0
        safe = jnp.where(nonzero, squared, 1.0)
        scaled = jnp.sqrt(safe) * thickness
        film = jnp.where(nonzero, (1.0 - jnp.exp(-scaled)) / scaled, 1.0)
        in_plane = (1.0 - film) / safe
        own_wave = jnp.where(quarter < 2, q_x, q_y)
        diag = jnp.where(paired, in_plane * own_wave * own_wave, film)
        sign = jnp.where(quarter % 2 == 0, -1.0, 1.0)
        mix = jnp.where(edge_x | edge_y | jnp.logical_not(paired), 0.0, sign * in_plane * q_x * q_y)
        diagonal[pl.ds(pl.multiple_of(256 * chunk, 256), 256), :] = diag * factor
        mix = (mix * factor).reshape(4, 2, 32, 128)[:, 0].reshape(128, 128)
        cross_term[pl.ds(pl.multiple_of(128 * chunk, 128), 128), :] = mix
        return carry

    lax.fori_loop(0, 4, build_tensor, 0)

    for copy in first_halo:
        copy.wait()
    coupling[8:16, :] = jnp.where(place > 0, coupling[8:16, :], 0.0)
    coupling[32:40, :] = jnp.where(place < SPACE - 1, coupling[32:40, :], 0.0)

    film_lane = lax.broadcasted_iota(jnp.int32, (8, GRID), 1)
    for g in range(4):
        top = 8 + 8 * g
        mid = coupling[top : top + 8, :]
        scaled = stiffness * mid
        up = scaled * coupling[top - 1 : top + 7, :]
        down = scaled * coupling[top + 1 : top + 9, :]
        left = jnp.where(film_lane == 0, 0.0, scaled * pltpu.roll(mid, 1, 1))
        right = jnp.where(film_lane == GRID - 1, 0.0, scaled * pltpu.roll(mid, GRID - 1, 1))
        rows = slice(8 * g, 8 * g + 8)
        weights[0, rows, :] = up
        weights[1, rows, :] = down
        weights[2, rows, :] = left
        weights[3, rows, :] = right
        weights[4, rows, :] = (up + down) + (left + right)

    def exchange(slot, g):
        top = 8 + 8 * g
        rows = slice(8 * g, 8 * g + 8)
        w = [weights[k, rows, :] for k in range(5)]
        magnet, result = [], []
        for c in range(3):
            mid = state[slot, c, top : top + 8, :]
            total = w[0] * state[slot, c, top - 1 : top + 7, :]
            total = total + w[1] * state[slot, c, top + 1 : top + 9, :]
            total = total + w[2] * pltpu.roll(mid, 1, 1)
            total = total + w[3] * pltpu.roll(mid, GRID - 1, 1)
            magnet.append(mid)
            result.append(total - w[4] * mid)
        return magnet, result

    def coarse_group(slot, g):
        magnet, effective = exchange(slot, g)
        rows = slice(8 * g, 8 * g + 8)
        effective = [effective[c] + field[c, rows, :] for c in range(3)]
        effective[2] = effective[2] - magnet[2]
        rate = torque(magnet, effective)
        return [magnet[c] + (FINE * step_time) * rate[c] for c in range(3)]

    def source_slot(n):
        return jnp.where(n == 0, 2, n % 2)

    def first_sweep(n, carry):
        for g in range(4):
            new = coarse_group(source_slot(n), g)
            for c in range(3):
                state[(n + 1) % 2, c, 8 + 8 * g : 16 + 8 * g, :] = new[c]
        return carry

    lax.fori_loop(0, slice_index, first_sweep, 0)
    start_slot = source_slot(slice_index)
    for g in (1, 2):
        new = coarse_group(start_slot, g)
        for c in range(3):
            coarse_end[c, 8 * g - 8 : 8 * g, :] = new[c]
    for c in range(3):
        start = state[start_slot, c, 16:32, :]
        base[c, :, :] = start
        slope[c, :, :] = jnp.zeros_like(start)
        state[0, c, 16:32, :] = start

    low_half = lax.broadcasted_iota(jnp.int32, (ROWS, 128), 1) < 64
    even_quarter = (lax.broadcasted_iota(jnp.int32, (128, 128), 1) // 32) % 2 == 0

    def partner(value):
        return jnp.where(even_quarter, pltpu.roll(value, 32, 1), pltpu.roll(value, 96, 1))

    def send_column(worker, target):
        return pltpu.make_async_remote_copy(
            src_ref=outgoing.at[worker],
            dst_ref=columns.at[pl.ds(pl.multiple_of(ROWS * place, ROWS), ROWS), :],
            send_sem=out_send, recv_sem=out_recv,
            device_id=device(slice_index, target), device_id_type=MESH,
        )

    def send_back(target):
        return pltpu.make_async_remote_copy(
            src_ref=answer.at[pl.ds(pl.multiple_of(ROWS * target, ROWS), ROWS), :],
            dst_ref=returned.at[rank],
            send_sem=back_send, recv_sem=back_recv,
            device_id=device(slice_index, target), device_id_type=MESH,
        )

    def planes_of(parts):
        return [(k, 1 if k == 1 else 0) for k in parts] + [(k, 0 if k == 1 else 1) for k in parts]

    def wait_bytes(ref, semaphore):
        pltpu.make_async_copy(ref, ref, semaphore).wait()

    def evaluation(e, carry):
        slot = e % 2
        for c in range(3):
            edges[c : c + 1, :] = state[0, c, 16:17, :]
            edges[3 + c : 4 + c, :] = state[0, c, 31:32, :]
        edge_copies = [
            pltpu.make_async_remote_copy(
                src_ref=edges, dst_ref=edge_in.at[slot, side],
                send_sem=edge_send.at[side], recv_sem=edge_recv.at[slot, side],
                device_id=device(slice_index, target), device_id_type=MESH,
            )
            for side, target in ((0, below), (1, above))
        ]
        for copy in edge_copies:
            copy.start()

        magnet = jnp.concatenate([state[0, c, 16:32, :] for c in range(3)], axis=0)
        high, low = split(magnet)
        stacked = jnp.concatenate([high, low], axis=0)
        for parts in ((2, 1, 3, 0),):
            for k in parts:
                part = (place_z // 2 + k) % 4
                cols = pl.ds(pl.multiple_of(256 * part, 256), 256)
                wide = dot(stacked, e1_high[:, cols])
                spectrum = wide[0:48] + wide[48:96] + dot(high, e1_low[:, cols])
                for half in range(2):
                    t = 2 * part + half
                    lanes = slice(128 * half, 128 * half + 128)
                    mx, my, mz = spectrum[0:16, lanes], spectrum[16:32, lanes], spectrum[32:48, lanes]
                    outgoing[2 * t] = jnp.where(low_half, mx, pltpu.roll(my, 64, 1))
                    outgoing[2 * t + 1] = jnp.where(low_half, pltpu.roll(mx, 64, 1), my)
                    outgoing[PAIRED + t] = mz
        for far in (4, 3, 2, 1, 0):
            for dy in (2, 1, -1, 0):
                for dz in (far, -far) if far in (1, 2, 3) else (far,):
                    sy = dy if dz >= 0 else -dy
                    if (dz, sy) != (0, 0):
                        plane = (place_z + dz) % 8
                        turn = (offset + sy - dz + 8) % 4

                        @pl.when(turn < 3)
                        def _(plane=plane, turn=turn, sy=sy):
                            send_column(number(plane, turn), 4 * plane + (place_y + sy) % 4).start()

        @pl.when(works)
        def _():
            columns[pl.ds(pl.multiple_of(ROWS * place, ROWS), ROWS), :] = outgoing[rank]

        for copy in edge_copies:
            copy.wait()
        for c in range(3):
            state[0, c, 15:16, :] = edge_in[slot, 0, 3 + c : 4 + c, :]
            state[0, c, 32:33, :] = edge_in[slot, 1, c : c + 1, :]
        for g in (1, 2):
            _, effective = exchange(0, g)
            for c in range(3):
                local_field[c, 8 * g - 8 : 8 * g, :] = effective[c] + field[c, 8 * g : 8 * g + 8, :]

        @pl.when(works)
        def _():
            wait_bytes(columns.at[pl.ds(0, ROWS * (SPACE - 1)), :], out_recv)
            column_high, column_low = split(columns[...])
            column_both = jnp.concatenate([column_high, column_low], axis=1)
            for part in range(4):
                rows = slice(256 * part, 256 * part + 256)
                wide = dot(e2_high[rows, :], column_both)
                spectrum = wide[:, 0:128] + wide[:, 128:256] + dot(e2_low[rows, :], column_high)
                spectrum = spectrum.reshape(4, 2, 32, 128)
                real = spectrum[:, 0].reshape(128, 128)
                imag = spectrum[:, 1].reshape(128, 128)
                diag = diagonal[rows, :].reshape(4, 2, 32, 128)
                mix = cross_term[128 * part : 128 * part + 128, :]
                real_out = diag[:, 0].reshape(128, 128) * real + mix * partner(imag)
                imag_out = diag[:, 1].reshape(128, 128) * imag - mix * partner(real)
                both = jnp.stack(
                    [real_out.reshape(4, 32, 128), imag_out.reshape(4, 32, 128)], axis=1
                ).reshape(256, 128)
                both_high, both_low = split(both)
                mixed[rows, 0:128] = both_high
                mixed[rows, 128:256] = both_low
            for parts in ((2,), (1, 3), (0,)):
                for k in parts:
                    rows = pl.ds(pl.multiple_of(128 * ((place_z // 2 + k) % 4), 128), 128)
                    wide = dot(e1_high[rows, :], mixed[...])
                    answer[rows, :] = wide[:, 0:128] + wide[:, 128:256] + dot(e1_low[rows, :], mixed[:, 0:128])
                for dy in (2, 1, -1, 0):
                    for k, half in planes_of(parts):
                        target = 4 * (2 * ((place_z // 2 + k) % 4) + half) + (place_y + dy) % 4
                        if k == 0 and dy == 0:

                            @pl.when(target != place)
                            def _(target=target):
                                send_back(target).start()

                        else:
                            send_back(target).start()

            returned[rank] = answer[pl.ds(pl.multiple_of(ROWS * place, ROWS), ROWS), :]
            wait_bytes(outgoing.at[pl.ds(0, WORKERS - 1)], out_send)
            wait_bytes(returned.at[pl.ds(0, WORKERS - 1)], back_recv)

        @pl.when(jnp.logical_not(works))
        def _():
            wait_bytes(outgoing, out_send)
            wait_bytes(returned, back_recv)

        parts = [[], [], []]
        for t in range(8):
            first, second = returned[2 * t], returned[2 * t + 1]
            parts[0].append(jnp.where(low_half, first, pltpu.roll(second, 64, 1)))
            parts[1].append(jnp.where(low_half, pltpu.roll(first, 64, 1), second))
            parts[2].append(returned[PAIRED + t])
        spectrum = jnp.concatenate([jnp.concatenate(part, axis=1) for part in parts], axis=0)
        spectrum_high, spectrum_low = split(spectrum)
        wide = dot(jnp.concatenate([spectrum_high, spectrum_low], axis=0), e2_high[...])
        demag = wide[0:48] + wide[48:96] + dot(spectrum_high, e2_low[...])

        corrects = slot == 1
        length = jnp.where(corrects, 0.5 * step_time, step_time)
        for g in range(2):
            rows = slice(8 * g, 8 * g + 8)
            here = [state[0, c, 16 + 8 * g : 24 + 8 * g, :] for c in range(3)]
            effective = [local_field[c, rows, :] + demag[16 * c + 8 * g : 16 * c + 8 * g + 8] for c in range(3)]
            rate = torque(here, effective)
            for c in range(3):
                start = base[c, rows, :]
                new = start + length * (slope[c, rows, :] + rate[c])
                state[0, c, 16 + 8 * g : 24 + 8 * g, :] = new
                slope[c, rows, :] = jnp.where(corrects, 0.0, rate[c])
                base[c, rows, :] = jnp.where(corrects, new, start)

        @pl.when(works)
        def _():
            wait_bytes(answer.at[pl.ds(0, ROWS * (SPACE - 1)), :], back_send)

        return carry

    lax.fori_loop(0, 2 * FINE, evaluation, 0)

    own = slice_index
    mate = own + 1 - 2 * core
    for c in range(3):
        jumps[own, c, 8:24, :] = state[0, c, 16:32, :] - coarse_end[c, :, :]

    def send_rows(i):
        return pltpu.make_async_remote_copy(
            src_ref=jumps.at[own, :, pl.ds(8, ROWS), :], dst_ref=jumps.at[own, :, pl.ds(8, ROWS), :],
            send_sem=gather_send.at[i], recv_sem=gather_recv.at[own],
            device_id=device(own + 2 * i, place), device_id_type=MESH,
        )

    def send_rims(n):
        return [
            pltpu.make_async_remote_copy(
                src_ref=jumps.at[n, :, pl.ds(source_row, 8), :], dst_ref=jumps.at[n, :, pl.ds(landing_row, 8), :],
                send_sem=rim_send.at[n, side], recv_sem=rim_recv.at[n, side],
                device_id=device(slice_index, target), device_id_type=MESH,
            )
            for side, target, source_row, landing_row in ((0, below, 16, 0), (1, above, 8, 24))
        ]

    def send_mate(n):
        return pltpu.make_async_remote_copy(
            src_ref=jumps.at[n], dst_ref=jumps.at[n],
            send_sem=forward_send.at[n], recv_sem=forward_recv.at[n],
            device_id=device(mate, place), device_id_type=MESH,
        )

    def holds(i):
        return core == 0 if i == 0 else chip >= i

    def start_rims(i):
        @pl.when(holds(i))
        def _():
            if i > 0:
                wait_bytes(jumps.at[own - 2 * i, :, pl.ds(8, ROWS), :], gather_recv.at[own - 2 * i])
            for copy in send_rims(own - 2 * i):
                copy.start()

    def pass_on(i):
        @pl.when(holds(i))
        def _():
            for copy in send_rims(own - 2 * i):
                copy.wait_recv()
            send_mate(own - 2 * i).start()

    start_rims(0)
    for i in (2, 3, 1):

        @pl.when(chip + i < TM // 2)
        def _(i=i):
            send_rows(i).start()

    start_rims(1)
    start_rims(3)
    start_rims(2)
    pass_on(0)
    pass_on(1)
    pass_on(3)

    def second_sweep(n, carry):
        @pl.when((chip >= 2) & (n == 2 * chip - 4))
        def _():
            pass_on(2)

        @pl.when(n % 2 != core)
        def _():
            wait_bytes(jumps.at[n], forward_recv.at[n])

        for g in range(4):
            new = coarse_group(source_slot(n), g)
            for c in range(3):
                state[(n + 1) % 2, c, 8 + 8 * g : 16 + 8 * g, :] = new[c] + jumps[n, c, 8 * g : 8 * g + 8, :]
        return carry

    lax.fori_loop(0, own, second_sweep, 0)
    for g in (1, 2):
        new = coarse_group(source_slot(own), g)
        for c in range(3):
            out[c, 8 * g - 8 : 8 * g, :] = new[c] + jumps[own, c, 8 * g : 8 * g + 8, :]

    for i in range(4):

        @pl.when(holds(i))
        def _(i=i):
            for copy in send_rims(own - 2 * i):
                copy.wait_send()
            send_mate(own - 2 * i).wait_send()

        if i > 0:

            @pl.when(chip + i < TM // 2)
            def _(i=i):
                send_rows(i).wait_send()


def solution(mesh):
    tables = twiddle_tables()
    vmem = pltpu.VMEM
    dma = pltpu.SemaphoreType.DMA
    scratch = [
        *[vmem(table.shape, F32) for table in tables],
        vmem((3, 3, 48, GRID), F32),
        vmem((3, 32, GRID), F32),
        vmem((48, GRID), F32),
        vmem((5, 32, GRID), F32),
        vmem((GRID, LENGTH), BF16),
        vmem((GRID, LENGTH), BF16),
        vmem((LENGTH, GRID), BF16),
        vmem((LENGTH, GRID), BF16),
        vmem((LENGTH, 128), F32),
        vmem((GRID, 128), F32),
        vmem((WORKERS, ROWS, 128), F32),
        vmem((GRID, 128), F32),
        vmem((LENGTH, 256), BF16),
        vmem((GRID, 128), F32),
        vmem((WORKERS, ROWS, 128), F32),
        vmem((8, GRID), F32),
        vmem((2, 2, 8, GRID), F32),
        vmem((3, ROWS, GRID), F32),
        vmem((3, ROWS, GRID), F32),
        vmem((3, ROWS, GRID), F32),
        vmem((3, ROWS, GRID), F32),
        vmem((TM, 3, 32, GRID), F32),
        dma((7,)),
        dma((2, 3)),
        dma((2, 3)),
        dma((2,)),
        dma((2, 2)),
        dma,
        dma,
        dma,
        dma,
        dma((4,)),
        dma((TM,)),
        dma((TM, 2)),
        dma((TM, 2)),
        dma((TM,)),
        dma((TM,)),
    ]

    def shards(initial_state, applied_field, coupling):
        by_component = [jnp.transpose(value, (1, 0, 2)) for value in (initial_state, applied_field)]
        result = pl.pallas_call(
            kernel,
            out_shape=pltpu.VMEM((3, ROWS, GRID), F32),
            in_specs=[pl.BlockSpec(memory_space=pl.ANY)] * 7,
            out_specs=pl.BlockSpec(memory_space=pltpu.VMEM),
            scratch_shapes=scratch,
            compiler_params=pltpu.CompilerParams(collective_id=0, has_side_effects=True),
        )(*by_component, coupling, *[jnp.asarray(table) for table in tables])
        return jnp.transpose(result, (1, 0, 2))[None]

    return jax.shard_map(
        shards,
        mesh=mesh,
        in_specs=(P("space", None, None), P("space", None, None), P("space", None)),
        out_specs=P("tm", "space", None, None),
        check_vma=False,
    )
```

```python
import math

import jax
import jax.numpy as jnp
import numpy as np
from jax import lax
from jax.experimental import pallas as pl
from jax.experimental.pallas import tpu as pltpu
from jax.sharding import PartitionSpec as P

MESH = pl.DeviceIdType.MESH
F32 = jnp.float32
BF16 = jnp.bfloat16

FINE = 2
step_time = 0.06
damping = 0.02
stiffness = 0.25
thickness = 8.0

GRID = 512
LENGTH = 2 * GRID
ROWS = 16
SPACE = 32
TM = 8
WORKERS = 24
PAIRED = 16


def twiddle_tables():
    unit = 2.0 * np.pi / LENGTH
    col = np.arange(LENGTH)
    wave = 32 * (col // 64) + col % 32
    kind = (col // 32) % 2
    phase = np.where(kind == 1, np.pi / 2, 0.0)
    nyquist = (kind == 1) & (wave == 0)
    wave = np.where(nyquist, GRID, wave)
    phase = np.where(nyquist, 0.0, phase)
    coarse = 16 * np.arange(GRID // 16)[:, None]
    fine = np.arange(16)[:, None]
    angle_coarse = unit * (coarse * wave % LENGTH)
    angle_fine = unit * (fine * wave % LENGTH) + phase
    x = np.arange(GRID)[None, :]
    block = 32 * np.arange(GRID // 32)[:, None]
    inner = np.arange(64)[:, None]
    angle_block = unit * (block * x % LENGTH)
    angle_inner = unit * (inner % 32 * x % LENGTH) + np.where(inner >= 32, np.pi / 2, 0.0)

    def both(angle):
        return np.concatenate([np.cos(angle), np.sin(angle)], axis=0).astype(np.float32)

    return both(angle_coarse), both(angle_fine), both(angle_block), both(angle_inner)


def split(value):
    high = value.astype(BF16)
    return high, (value - high.astype(F32)).astype(BF16)


def dot(left, right):
    return jnp.dot(left, right, preferred_element_type=F32)


def cross(a, b):
    return [
        a[1] * b[2] - a[2] * b[1],
        a[2] * b[0] - a[0] * b[2],
        a[0] * b[1] - a[1] * b[0],
    ]


def torque(magnet, effective):
    first = cross(magnet, effective)
    second = cross(magnet, first)
    scale = -1.0 / (1.0 + damping * damping)
    return [scale * (f + damping * s) for f, s in zip(first, second)]


def kernel(
    state_in, field_in, coupling_in, coarse_in, fine_in, block_in, inner_in, out,
    t_coarse, t_fine, t_block, t_inner, state, field, coupling, weights, e1_high, e1_low, e2_high, e2_low, diagonal, cross_term,
    outgoing, columns, mixed, answer, returned, edges, edge_in, base, slope, local_field, coarse_end, jumps,
    load, halo_send, halo_recv, edge_send, edge_recv, out_send, out_recv, back_send, back_recv,
    gather_send, gather_recv, rim_send, rim_recv, forward_send, forward_recv,
):
    slice_index = lax.axis_index("tm")
    place = lax.axis_index("space")

    def device(which_slice, which_place):
        return (which_slice, which_place)

    chip = slice_index // 2
    core = slice_index % 2
    above = (place + SPACE - 1) % SPACE
    below = (place + 1) % SPACE
    offset = (place % 4 - (place // 4) % 4 + 3) % 4
    works = offset < 3

    def number(plane, turn):
        return jnp.where(turn < 2, 2 * plane + turn, PAIRED + plane)

    rank = number(place // 4, jnp.minimum(offset, 2))

    place_z, place_y = place // 4, place % 4

    loads = [
        pltpu.make_async_copy(source, landing, load.at[i])
        for i, (source, landing) in enumerate(
            (
                (state_in, state.at[2, :, pl.ds(16, ROWS), :]),
                (field_in, field.at[:, pl.ds(8, ROWS), :]),
                (coupling_in, coupling.at[pl.ds(16, ROWS), :]),
                (coarse_in, t_coarse),
                (fine_in, t_fine),
                (block_in, t_block),
                (inner_in, t_inner),
            )
        )
    ]
    for copy in loads:
        copy.start()

    barrier = pltpu.get_barrier_semaphore()

    def greet_space(i, carry):
        pl.semaphore_signal(barrier, inc=1, device_id=device(slice_index, (place + i) % SPACE), device_id_type=MESH)
        return carry

    def greet_tm(i, carry):
        pl.semaphore_signal(barrier, inc=1, device_id=device((slice_index + i) % TM, place), device_id_type=MESH)
        return carry

    lax.fori_loop(1, SPACE, greet_space, 0)
    lax.fori_loop(1, TM, greet_tm, 0)

    zero_rows = jnp.zeros((8, GRID), F32)
    for c in range(3):
        for slot in range(3):
            state[slot, c, 0:8, :] = zero_rows
            state[slot, c, 40:48, :] = zero_rows
    coupling[0:8, :] = zero_rows
    coupling[40:48, :] = zero_rows
    edges[...] = zero_rows

    for copy in loads[:3]:
        copy.wait()
    pl.semaphore_wait(barrier, SPACE - 1 + TM - 1)

    def halo_copies():
        copies = []
        for side, target, source_row, landing_row in ((0, below, 24, 8), (1, above, 16, 32)):
            for what, (source, landing) in enumerate(
                (
                    (state.at[2, :, pl.ds(source_row, 8), :], state.at[2, :, pl.ds(landing_row, 8), :]),
                    (field.at[:, pl.ds(source_row - 8, 8), :], field.at[:, pl.ds(landing_row - 8, 8), :]),
                    (coupling.at[pl.ds(source_row, 8), :], coupling.at[pl.ds(landing_row, 8), :]),
                )
            ):
                copies.append(
                    pltpu.make_async_remote_copy(
                        src_ref=source, dst_ref=landing,
                        send_sem=halo_send.at[side, what], recv_sem=halo_recv.at[side, what],
                        device_id=device(slice_index, target), device_id_type=MESH,
                    )
                )
        return copies

    first_halo = halo_copies()
    for copy in first_halo:
        copy.start()

    for copy in loads[3:]:
        copy.wait()

    def build_e1(a, carry):
        value = t_coarse[pl.ds(a, 1), :] * t_fine[0:16, :] - t_coarse[pl.ds(32 + a, 1), :] * t_fine[16:32, :]
        high, low = split(value)
        rows = pl.ds(pl.multiple_of(16 * a, 16), 16)
        e1_high[rows, :] = high
        e1_low[rows, :] = low
        return carry

    lax.fori_loop(0, GRID // 16, build_e1, 0)
    inner_row = lax.broadcasted_iota(jnp.int32, (64, GRID), 0)
    inner_lane = lax.broadcasted_iota(jnp.int32, (64, GRID), 1)
    alternating = (1 - 2 * (inner_lane % 2)).astype(F32)

    def build_e2(j, carry):
        value = t_block[pl.ds(j, 1), :] * t_inner[0:64, :] - t_block[pl.ds(16 + j, 1), :] * t_inner[64:128, :]
        value = jnp.where((inner_row == 32) & (j == 0), alternating, value)
        high, low = split(value)
        rows = pl.ds(pl.multiple_of(64 * j, 64), 64)
        e2_high[rows, :] = high
        e2_low[rows, :] = low
        return carry

    lax.fori_loop(0, GRID // 32, build_e2, 0)

    def build_tensor(chunk, carry):
        row = 256 * chunk + lax.broadcasted_iota(jnp.int32, (256, 128), 0)
        lane = lax.broadcasted_iota(jnp.int32, (256, 128), 1)
        quarter = lane // 32
        paired = rank < PAIRED
        wave_y = 32 * (row // 64) + row % 32
        wave_y = jnp.where((wave_y == 0) & ((row // 32) % 2 == 1), GRID, wave_y)
        first_x = jnp.where(paired, 32 * rank, 64 * (rank - PAIRED) + 32 * (quarter // 2))
        wave_x = first_x + lane % 32
        wave_x = jnp.where((wave_x == 0) & (quarter % 2 == 1), GRID, wave_x)
        edge_x = (wave_x == 0) | (wave_x == GRID)
        edge_y = (wave_y == 0) | (wave_y == GRID)
        factor = jnp.where(edge_x, 1.0, 2.0) * jnp.where(edge_y, 1.0, 2.0) * (-1.0 / (LENGTH * LENGTH))
        q_x = wave_x.astype(F32) * (2.0 * math.pi / LENGTH)
        q_y = wave_y.astype(F32) * (2.0 * math.pi / LENGTH)
        squared = q_x * q_x + q_y * q_y
        nonzero = (wave_x + wave_y) > 0
        safe = jnp.where(nonzero, squared, 1.0)
        scaled = jnp.sqrt(safe) * thickness
        film = jnp.where(nonzero, (1.0 - jnp.exp(-scaled)) / scaled, 1.0)
        in_plane = (1.0 - film) / safe
        own_wave = jnp.where(quarter < 2, q_x, q_y)
        diag = jnp.where(paired, in_plane * own_wave * own_wave, film)
        sign = jnp.where(quarter % 2 == 0, -1.0, 1.0)
        mix = jnp.where(edge_x | edge_y | jnp.logical_not(paired), 0.0, sign * in_plane * q_x * q_y)
        diagonal[pl.ds(pl.multiple_of(256 * chunk, 256), 256), :] = diag * factor
        mix = (mix * factor).reshape(4, 2, 32, 128)[:, 0].reshape(128, 128)
        cross_term[pl.ds(pl.multiple_of(128 * chunk, 128), 128), :] = mix
        return carry

    lax.fori_loop(0, 4, build_tensor, 0)

    for copy in first_halo:
        copy.wait()
    coupling[8:16, :] = jnp.where(place > 0, coupling[8:16, :], 0.0)
    coupling[32:40, :] = jnp.where(place < SPACE - 1, coupling[32:40, :], 0.0)

    film_lane = lax.broadcasted_iota(jnp.int32, (8, GRID), 1)
    for g in range(4):
        top = 8 + 8 * g
        mid = coupling[top : top + 8, :]
        scaled = stiffness * mid
        up = scaled * coupling[top - 1 : top + 7, :]
        down = scaled * coupling[top + 1 : top + 9, :]
        left = jnp.where(film_lane == 0, 0.0, scaled * pltpu.roll(mid, 1, 1))
        right = jnp.where(film_lane == GRID - 1, 0.0, scaled * pltpu.roll(mid, GRID - 1, 1))
        rows = slice(8 * g, 8 * g + 8)
        weights[0, rows, :] = up
        weights[1, rows, :] = down
        weights[2, rows, :] = left
        weights[3, rows, :] = right
        weights[4, rows, :] = (up + down) + (left + right)

    def exchange(slot, g):
        top = 8 + 8 * g
        rows = slice(8 * g, 8 * g + 8)
        w = [weights[k, rows, :] for k in range(5)]
        magnet, result = [], []
        for c in range(3):
            mid = state[slot, c, top : top + 8, :]
            total = w[0] * state[slot, c, top - 1 : top + 7, :]
            total = total + w[1] * state[slot, c, top + 1 : top + 9, :]
            total = total + w[2] * pltpu.roll(mid, 1, 1)
            total = total + w[3] * pltpu.roll(mid, GRID - 1, 1)
            magnet.append(mid)
            result.append(total - w[4] * mid)
        return magnet, result

    def coarse_group(slot, g):
        magnet, effective = exchange(slot, g)
        rows = slice(8 * g, 8 * g + 8)
        effective = [effective[c] + field[c, rows, :] for c in range(3)]
        effective[2] = effective[2] - magnet[2]
        rate = torque(magnet, effective)
        return [magnet[c] + (FINE * step_time) * rate[c] for c in range(3)]

    def source_slot(n):
        return jnp.where(n == 0, 2, n % 2)

    def first_sweep(n, carry):
        for g in range(4):
            new = coarse_group(source_slot(n), g)
            for c in range(3):
                state[(n + 1) % 2, c, 8 + 8 * g : 16 + 8 * g, :] = new[c]
        return carry

    lax.fori_loop(0, slice_index, first_sweep, 0)
    start_slot = source_slot(slice_index)
    for g in (1, 2):
        new = coarse_group(start_slot, g)
        for c in range(3):
            coarse_end[c, 8 * g - 8 : 8 * g, :] = new[c]
    for c in range(3):
        start = state[start_slot, c, 16:32, :]
        base[c, :, :] = start
        slope[c, :, :] = jnp.zeros_like(start)
        state[0, c, 16:32, :] = start

    low_half = lax.broadcasted_iota(jnp.int32, (ROWS, 128), 1) < 64
    even_quarter = (lax.broadcasted_iota(jnp.int32, (128, 128), 1) // 32) % 2 == 0

    def partner(value):
        return jnp.where(even_quarter, pltpu.roll(value, 32, 1), pltpu.roll(value, 96, 1))

    def send_column(worker, target):
        return pltpu.make_async_remote_copy(
            src_ref=outgoing.at[worker],
            dst_ref=columns.at[pl.ds(pl.multiple_of(ROWS * place, ROWS), ROWS), :],
            send_sem=out_send, recv_sem=out_recv,
            device_id=device(slice_index, target), device_id_type=MESH,
        )

    def send_back(target):
        return pltpu.make_async_remote_copy(
            src_ref=answer.at[pl.ds(pl.multiple_of(ROWS * target, ROWS), ROWS), :],
            dst_ref=returned.at[rank],
            send_sem=back_send, recv_sem=back_recv,
            device_id=device(slice_index, target), device_id_type=MESH,
        )

    def planes_of(parts):
        return [(k, 1 if k == 1 else 0) for k in parts] + [(k, 0 if k == 1 else 1) for k in parts]

    def wait_bytes(ref, semaphore):
        pltpu.make_async_copy(ref, ref, semaphore).wait()

    def evaluation(e, carry):
        slot = e % 2
        for c in range(3):
            edges[c : c + 1, :] = state[0, c, 16:17, :]
            edges[3 + c : 4 + c, :] = state[0, c, 31:32, :]
        edge_copies = [
            pltpu.make_async_remote_copy(
                src_ref=edges, dst_ref=edge_in.at[slot, side],
                send_sem=edge_send.at[side], recv_sem=edge_recv.at[slot, side],
                device_id=device(slice_index, target), device_id_type=MESH,
            )
            for side, target in ((0, below), (1, above))
        ]
        for copy in edge_copies:
            copy.start()

        magnet = jnp.concatenate([state[0, c, 16:32, :] for c in range(3)], axis=0)
        high, low = split(magnet)
        stacked = jnp.concatenate([high, low], axis=0)
        for parts in ((2, 1, 3, 0),):
            for k in parts:
                part = (place_z // 2 + k) % 4
                cols = pl.ds(pl.multiple_of(256 * part, 256), 256)
                wide = dot(stacked, e1_high[:, cols])
                spectrum = wide[0:48] + wide[48:96] + dot(high, e1_low[:, cols])
                for half in range(2):
                    t = 2 * part + half
                    lanes = slice(128 * half, 128 * half + 128)
                    mx, my, mz = spectrum[0:16, lanes], spectrum[16:32, lanes], spectrum[32:48, lanes]
                    outgoing[2 * t] = jnp.where(low_half, mx, pltpu.roll(my, 64, 1))
                    outgoing[2 * t + 1] = jnp.where(low_half, pltpu.roll(mx, 64, 1), my)
                    outgoing[PAIRED + t] = mz
        for far in (4, 3, 2, 1, 0):
            for dy in (2, 1, -1, 0):
                for dz in (far, -far) if far in (1, 2, 3) else (far,):
                    sy = dy if dz >= 0 else -dy
                    if (dz, sy) != (0, 0):
                        plane = (place_z + dz) % 8
                        turn = (offset + sy - dz + 8) % 4

                        @pl.when(turn < 3)
                        def _(plane=plane, turn=turn, sy=sy):
                            send_column(number(plane, turn), 4 * plane + (place_y + sy) % 4).start()

        @pl.when(works)
        def _():
            columns[pl.ds(pl.multiple_of(ROWS * place, ROWS), ROWS), :] = outgoing[rank]

        for copy in edge_copies:
            copy.wait()
        for c in range(3):
            state[0, c, 15:16, :] = edge_in[slot, 0, 3 + c : 4 + c, :]
            state[0, c, 32:33, :] = edge_in[slot, 1, c : c + 1, :]
        for g in (1, 2):
            _, effective = exchange(0, g)
            for c in range(3):
                local_field[c, 8 * g - 8 : 8 * g, :] = effective[c] + field[c, 8 * g : 8 * g + 8, :]

        @pl.when(works)
        def _():
            wait_bytes(columns.at[pl.ds(0, ROWS * (SPACE - 1)), :], out_recv)
            column_high, column_low = split(columns[...])
            column_both = jnp.concatenate([column_high, column_low], axis=1)
            for part in range(4):
                rows = slice(256 * part, 256 * part + 256)
                wide = dot(e2_high[rows, :], column_both)
                spectrum = wide[:, 0:128] + wide[:, 128:256] + dot(e2_low[rows, :], column_high)
                spectrum = spectrum.reshape(4, 2, 32, 128)
                real = spectrum[:, 0].reshape(128, 128)
                imag = spectrum[:, 1].reshape(128, 128)
                diag = diagonal[rows, :].reshape(4, 2, 32, 128)
                mix = cross_term[128 * part : 128 * part + 128, :]
                real_out = diag[:, 0].reshape(128, 128) * real + mix * partner(imag)
                imag_out = diag[:, 1].reshape(128, 128) * imag - mix * partner(real)
                both = jnp.stack(
                    [real_out.reshape(4, 32, 128), imag_out.reshape(4, 32, 128)], axis=1
                ).reshape(256, 128)
                both_high, both_low = split(both)
                mixed[rows, 0:128] = both_high
                mixed[rows, 128:256] = both_low
            for parts in ((2,), (1, 3), (0,)):
                for k in parts:
                    rows = pl.ds(pl.multiple_of(128 * ((place_z // 2 + k) % 4), 128), 128)
                    wide = dot(e1_high[rows, :], mixed[...])
                    answer[rows, :] = wide[:, 0:128] + wide[:, 128:256] + dot(e1_low[rows, :], mixed[:, 0:128])
                for dy in (2, 1, -1, 0):
                    for k, half in planes_of(parts):
                        target = 4 * (2 * ((place_z // 2 + k) % 4) + half) + (place_y + dy) % 4
                        if k == 0 and dy == 0:

                            @pl.when(target != place)
                            def _(target=target):
                                send_back(target).start()

                        else:
                            send_back(target).start()

            returned[rank] = answer[pl.ds(pl.multiple_of(ROWS * place, ROWS), ROWS), :]
            wait_bytes(outgoing.at[pl.ds(0, WORKERS - 1)], out_send)
            wait_bytes(returned.at[pl.ds(0, WORKERS - 1)], back_recv)

        @pl.when(jnp.logical_not(works))
        def _():
            wait_bytes(outgoing, out_send)
            wait_bytes(returned, back_recv)

        parts = [[], [], []]
        for t in range(8):
            first, second = returned[2 * t], returned[2 * t + 1]
            parts[0].append(jnp.where(low_half, first, pltpu.roll(second, 64, 1)))
            parts[1].append(jnp.where(low_half, pltpu.roll(first, 64, 1), second))
            parts[2].append(returned[PAIRED + t])
        spectrum = jnp.concatenate([jnp.concatenate(part, axis=1) for part in parts], axis=0)
        spectrum_high, spectrum_low = split(spectrum)
        wide = dot(jnp.concatenate([spectrum_high, spectrum_low], axis=0), e2_high[...])
        demag = wide[0:48] + wide[48:96] + dot(spectrum_high, e2_low[...])

        corrects = slot == 1
        length = jnp.where(corrects, 0.5 * step_time, step_time)
        for g in range(2):
            rows = slice(8 * g, 8 * g + 8)
            here = [state[0, c, 16 + 8 * g : 24 + 8 * g, :] for c in range(3)]
            effective = [local_field[c, rows, :] + demag[16 * c + 8 * g : 16 * c + 8 * g + 8] for c in range(3)]
            rate = torque(here, effective)
            for c in range(3):
                start = base[c, rows, :]
                new = start + length * (slope[c, rows, :] + rate[c])
                state[0, c, 16 + 8 * g : 24 + 8 * g, :] = new
                slope[c, rows, :] = jnp.where(corrects, 0.0, rate[c])
                base[c, rows, :] = jnp.where(corrects, new, start)

        @pl.when(works)
        def _():
            wait_bytes(answer.at[pl.ds(0, ROWS * (SPACE - 1)), :], back_send)

        return carry

    lax.fori_loop(0, 2 * FINE, evaluation, 0)

    own = slice_index
    mate = own + 1 - 2 * core
    for c in range(3):
        jumps[own, c, 8:24, :] = state[0, c, 16:32, :] - coarse_end[c, :, :]

    def send_rows(i):
        return pltpu.make_async_remote_copy(
            src_ref=jumps.at[own, :, pl.ds(8, ROWS), :], dst_ref=jumps.at[own, :, pl.ds(8, ROWS), :],
            send_sem=gather_send.at[i], recv_sem=gather_recv.at[own],
            device_id=device(own + 2 * i, place), device_id_type=MESH,
        )

    def send_rims(i):
        n, depth = own - 2 * i, 2 * i + 1
        return [
            pltpu.make_async_remote_copy(
                src_ref=jumps.at[n, :, pl.ds(source_row, depth), :], dst_ref=jumps.at[n, :, pl.ds(landing_row, depth), :],
                send_sem=rim_send.at[n, side], recv_sem=rim_recv.at[n, side],
                device_id=device(slice_index, target), device_id_type=MESH,
            )
            for side, target, source_row, landing_row in ((0, below, 24 - depth, 8 - depth), (1, above, 8, 24))
        ]

    def send_mate(n):
        return pltpu.make_async_remote_copy(
            src_ref=jumps.at[n], dst_ref=jumps.at[n],
            send_sem=forward_send.at[n], recv_sem=forward_recv.at[n],
            device_id=device(mate, place), device_id_type=MESH,
        )

    def holds(i):
        return core == 0 if i == 0 else chip >= i

    def start_rims(i):
        @pl.when(holds(i))
        def _():
            if i > 0:
                wait_bytes(jumps.at[own - 2 * i, :, pl.ds(8, ROWS), :], gather_recv.at[own - 2 * i])
            for copy in send_rims(i):
                copy.start()

    def pass_on(i):
        @pl.when(holds(i))
        def _():
            for copy in send_rims(i):
                copy.wait_recv()
            send_mate(own - 2 * i).start()

    start_rims(0)
    for i in (2, 3, 1):

        @pl.when(chip + i < TM // 2)
        def _(i=i):
            send_rows(i).start()

    start_rims(1)
    start_rims(3)
    start_rims(2)
    pass_on(0)
    pass_on(1)
    pass_on(3)

    def second_sweep(n, carry):
        @pl.when((chip >= 2) & (n == 2 * chip - 4))
        def _():
            pass_on(2)

        @pl.when(n % 2 != core)
        def _():
            wait_bytes(jumps.at[n], forward_recv.at[n])

        for g in range(4):
            new = coarse_group(source_slot(n), g)
            for c in range(3):
                state[(n + 1) % 2, c, 8 + 8 * g : 16 + 8 * g, :] = new[c] + jumps[n, c, 8 * g : 8 * g + 8, :]
        return carry

    lax.fori_loop(0, own, second_sweep, 0)
    for g in (1, 2):
        new = coarse_group(source_slot(own), g)
        for c in range(3):
            out[c, 8 * g - 8 : 8 * g, :] = new[c] + jumps[own, c, 8 * g : 8 * g + 8, :]

    for i in range(4):

        @pl.when(holds(i))
        def _(i=i):
            for copy in send_rims(i):
                copy.wait_send()
            send_mate(own - 2 * i).wait_send()

        if i > 0:

            @pl.when(chip + i < TM // 2)
            def _(i=i):
                send_rows(i).wait_send()


def solution(mesh):
    tables = twiddle_tables()
    vmem = pltpu.VMEM
    dma = pltpu.SemaphoreType.DMA
    scratch = [
        *[vmem(table.shape, F32) for table in tables],
        vmem((3, 3, 48, GRID), F32),
        vmem((3, 32, GRID), F32),
        vmem((48, GRID), F32),
        vmem((5, 32, GRID), F32),
        vmem((GRID, LENGTH), BF16),
        vmem((GRID, LENGTH), BF16),
        vmem((LENGTH, GRID), BF16),
        vmem((LENGTH, GRID), BF16),
        vmem((LENGTH, 128), F32),
        vmem((GRID, 128), F32),
        vmem((WORKERS, ROWS, 128), F32),
        vmem((GRID, 128), F32),
        vmem((LENGTH, 256), BF16),
        vmem((GRID, 128), F32),
        vmem((WORKERS, ROWS, 128), F32),
        vmem((8, GRID), F32),
        vmem((2, 2, 8, GRID), F32),
        vmem((3, ROWS, GRID), F32),
        vmem((3, ROWS, GRID), F32),
        vmem((3, ROWS, GRID), F32),
        vmem((3, ROWS, GRID), F32),
        vmem((TM, 3, 32, GRID), F32),
        dma((7,)),
        dma((2, 3)),
        dma((2, 3)),
        dma((2,)),
        dma((2, 2)),
        dma,
        dma,
        dma,
        dma,
        dma((4,)),
        dma((TM,)),
        dma((TM, 2)),
        dma((TM, 2)),
        dma((TM,)),
        dma((TM,)),
    ]

    def shards(initial_state, applied_field, coupling):
        by_component = [jnp.transpose(value, (1, 0, 2)) for value in (initial_state, applied_field)]
        result = pl.pallas_call(
            kernel,
            out_shape=pltpu.VMEM((3, ROWS, GRID), F32),
            in_specs=[pl.BlockSpec(memory_space=pl.ANY)] * 7,
            out_specs=pl.BlockSpec(memory_space=pltpu.VMEM),
            scratch_shapes=scratch,
            compiler_params=pltpu.CompilerParams(collective_id=0, has_side_effects=True),
        )(*by_component, coupling, *[jnp.asarray(table) for table in tables])
        return jnp.transpose(result, (1, 0, 2))[None]

    return jax.shard_map(
        shards,
        mesh=mesh,
        in_specs=(P("space", None, None), P("space", None, None), P("space", None)),
        out_specs=P("tm", "space", None, None),
        check_vma=False,
    )
```

```python
import math

import jax
import jax.numpy as jnp
import numpy as np
from jax import lax
from jax.experimental import pallas as pl
from jax.experimental.pallas import tpu as pltpu
from jax.sharding import PartitionSpec as P

MESH = pl.DeviceIdType.MESH
F32 = jnp.float32
BF16 = jnp.bfloat16

FINE = 2
step_time = 0.06
damping = 0.02
stiffness = 0.25
thickness = 8.0

GRID = 512
LENGTH = 2 * GRID
ROWS = 16
SPACE = 32
TM = 8
WORKERS = 24
PAIRED = 16


def twiddle_tables():
    unit = 2.0 * np.pi / LENGTH
    col = np.arange(LENGTH)
    wave = 32 * (col // 64) + col % 32
    kind = (col // 32) % 2
    phase = np.where(kind == 1, np.pi / 2, 0.0)
    nyquist = (kind == 1) & (wave == 0)
    wave = np.where(nyquist, GRID, wave)
    phase = np.where(nyquist, 0.0, phase)
    coarse = 16 * np.arange(GRID // 16)[:, None]
    fine = np.arange(16)[:, None]
    angle_coarse = unit * (coarse * wave % LENGTH)
    angle_fine = unit * (fine * wave % LENGTH) + phase
    x = np.arange(GRID)[None, :]
    block = 32 * np.arange(GRID // 32)[:, None]
    inner = np.arange(64)[:, None]
    angle_block = unit * (block * x % LENGTH)
    angle_inner = unit * (inner % 32 * x % LENGTH) + np.where(inner >= 32, np.pi / 2, 0.0)

    def both(angle):
        return np.concatenate([np.cos(angle), np.sin(angle)], axis=0).astype(np.float32)

    return both(angle_coarse), both(angle_fine), both(angle_block), both(angle_inner)


def split(value):
    high = value.astype(BF16)
    return high, (value - high.astype(F32)).astype(BF16)


def dot(left, right):
    return jnp.dot(left, right, preferred_element_type=F32)


def cross(a, b):
    return [
        a[1] * b[2] - a[2] * b[1],
        a[2] * b[0] - a[0] * b[2],
        a[0] * b[1] - a[1] * b[0],
    ]


def torque(magnet, effective):
    first = cross(magnet, effective)
    second = cross(magnet, first)
    scale = -1.0 / (1.0 + damping * damping)
    return [scale * (f + damping * s) for f, s in zip(first, second)]


def kernel(
    state_in, field_in, coupling_in, coarse_in, fine_in, block_in, inner_in, out,
    t_coarse, t_fine, t_block, t_inner, state, field, coupling, weights, e1_high, e1_low, e2_high, e2_low, diagonal, cross_term,
    outgoing, columns, mixed, answer, returned, edges, edge_in, base, slope, local_field, coarse_end, jumps,
    load, halo_send, halo_recv, edge_send, edge_recv, out_send, out_recv, back_send, back_recv,
    gather_send, gather_recv, rim_send, rim_recv, forward_send, forward_recv,
):
    slice_index = lax.axis_index("tm")
    place = lax.axis_index("space")

    def device(which_slice, which_place):
        return (which_slice, which_place)

    chip = slice_index // 2
    core = slice_index % 2
    above = (place + SPACE - 1) % SPACE
    below = (place + 1) % SPACE
    offset = (place % 4 - (place // 4) % 4 + 3) % 4
    works = offset < 3

    def number(plane, turn):
        return jnp.where(turn < 2, 2 * plane + turn, PAIRED + plane)

    rank = number(place // 4, jnp.minimum(offset, 2))

    place_z, place_y = place // 4, place % 4

    loads = [
        pltpu.make_async_copy(source, landing, load.at[i])
        for i, (source, landing) in enumerate(
            (
                (state_in, state.at[2, :, pl.ds(16, ROWS), :]),
                (field_in, field.at[:, pl.ds(8, ROWS), :]),
                (coupling_in, coupling.at[pl.ds(16, ROWS), :]),
                (coarse_in, t_coarse),
                (fine_in, t_fine),
                (block_in, t_block),
                (inner_in, t_inner),
            )
        )
    ]
    for copy in loads:
        copy.start()

    barrier = pltpu.get_barrier_semaphore()

    def far_first(i):
        step = jnp.where(i % 2 == 0, SPACE - i // 2, (i + 1) // 2)
        return (place + SPACE // 2 + jnp.where(i == SPACE - 1, 0, step)) % SPACE

    def greet_space(i, carry):
        pl.semaphore_signal(barrier, inc=1, device_id=device(slice_index, far_first(i)), device_id_type=MESH)
        return carry

    def greet_tm(i, carry):
        pl.semaphore_signal(barrier, inc=1, device_id=device((slice_index + i) % TM, place), device_id_type=MESH)
        return carry

    lax.fori_loop(1, SPACE, greet_space, 0)
    lax.fori_loop(1, TM, greet_tm, 0)

    zero_rows = jnp.zeros((8, GRID), F32)
    for c in range(3):
        for slot in range(3):
            state[slot, c, 0:8, :] = zero_rows
            state[slot, c, 40:48, :] = zero_rows
    coupling[0:8, :] = zero_rows
    coupling[40:48, :] = zero_rows
    edges[...] = zero_rows

    for copy in loads[:3]:
        copy.wait()
    pl.semaphore_wait(barrier, SPACE - 1 + TM - 1)

    def halo_copies():
        copies = []
        for side, target, source_row, landing_row in ((0, below, 24, 8), (1, above, 16, 32)):
            for what, (source, landing) in enumerate(
                (
                    (state.at[2, :, pl.ds(source_row, 8), :], state.at[2, :, pl.ds(landing_row, 8), :]),
                    (field.at[:, pl.ds(source_row - 8, 8), :], field.at[:, pl.ds(landing_row - 8, 8), :]),
                    (coupling.at[pl.ds(source_row, 8), :], coupling.at[pl.ds(landing_row, 8), :]),
                )
            ):
                copies.append(
                    pltpu.make_async_remote_copy(
                        src_ref=source, dst_ref=landing,
                        send_sem=halo_send.at[side, what], recv_sem=halo_recv.at[side, what],
                        device_id=device(slice_index, target), device_id_type=MESH,
                    )
                )
        return copies

    first_halo = halo_copies()
    for copy in first_halo:
        copy.start()

    for copy in loads[3:]:
        copy.wait()

    def build_e1(a, carry):
        value = t_coarse[pl.ds(a, 1), :] * t_fine[0:16, :] - t_coarse[pl.ds(32 + a, 1), :] * t_fine[16:32, :]
        high, low = split(value)
        rows = pl.ds(pl.multiple_of(16 * a, 16), 16)
        e1_high[rows, :] = high
        e1_low[rows, :] = low
        return carry

    lax.fori_loop(0, GRID // 16, build_e1, 0)
    inner_row = lax.broadcasted_iota(jnp.int32, (64, GRID), 0)
    inner_lane = lax.broadcasted_iota(jnp.int32, (64, GRID), 1)
    alternating = (1 - 2 * (inner_lane % 2)).astype(F32)

    def build_e2(j, carry):
        value = t_block[pl.ds(j, 1), :] * t_inner[0:64, :] - t_block[pl.ds(16 + j, 1), :] * t_inner[64:128, :]
        value = jnp.where((inner_row == 32) & (j == 0), alternating, value)
        high, low = split(value)
        rows = pl.ds(pl.multiple_of(64 * j, 64), 64)
        e2_high[rows, :] = high
        e2_low[rows, :] = low
        return carry

    lax.fori_loop(0, GRID // 32, build_e2, 0)

    def build_tensor(chunk, carry):
        row = 256 * chunk + lax.broadcasted_iota(jnp.int32, (256, 128), 0)
        lane = lax.broadcasted_iota(jnp.int32, (256, 128), 1)
        quarter = lane // 32
        paired = rank < PAIRED
        wave_y = 32 * (row // 64) + row % 32
        wave_y = jnp.where((wave_y == 0) & ((row // 32) % 2 == 1), GRID, wave_y)
        first_x = jnp.where(paired, 32 * rank, 64 * (rank - PAIRED) + 32 * (quarter // 2))
        wave_x = first_x + lane % 32
        wave_x = jnp.where((wave_x == 0) & (quarter % 2 == 1), GRID, wave_x)
        edge_x = (wave_x == 0) | (wave_x == GRID)
        edge_y = (wave_y == 0) | (wave_y == GRID)
        factor = jnp.where(edge_x, 1.0, 2.0) * jnp.where(edge_y, 1.0, 2.0) * (-1.0 / (LENGTH * LENGTH))
        q_x = wave_x.astype(F32) * (2.0 * math.pi / LENGTH)
        q_y = wave_y.astype(F32) * (2.0 * math.pi / LENGTH)
        squared = q_x * q_x + q_y * q_y
        nonzero = (wave_x + wave_y) > 0
        safe = jnp.where(nonzero, squared, 1.0)
        scaled = jnp.sqrt(safe) * thickness
        film = jnp.where(nonzero, (1.0 - jnp.exp(-scaled)) / scaled, 1.0)
        in_plane = (1.0 - film) / safe
        own_wave = jnp.where(quarter < 2, q_x, q_y)
        diag = jnp.where(paired, in_plane * own_wave * own_wave, film)
        sign = jnp.where(quarter % 2 == 0, -1.0, 1.0)
        mix = jnp.where(edge_x | edge_y | jnp.logical_not(paired), 0.0, sign * in_plane * q_x * q_y)
        diagonal[pl.ds(pl.multiple_of(256 * chunk, 256), 256), :] = diag * factor
        mix = (mix * factor).reshape(4, 2, 32, 128)[:, 0].reshape(128, 128)
        cross_term[pl.ds(pl.multiple_of(128 * chunk, 128), 128), :] = mix
        return carry

    lax.fori_loop(0, 4, build_tensor, 0)

    for copy in first_halo:
        copy.wait()
    coupling[8:16, :] = jnp.where(place > 0, coupling[8:16, :], 0.0)
    coupling[32:40, :] = jnp.where(place < SPACE - 1, coupling[32:40, :], 0.0)

    film_lane = lax.broadcasted_iota(jnp.int32, (8, GRID), 1)
    for g in range(4):
        top = 8 + 8 * g
        mid = coupling[top : top + 8, :]
        scaled = stiffness * mid
        up = scaled * coupling[top - 1 : top + 7, :]
        down = scaled * coupling[top + 1 : top + 9, :]
        left = jnp.where(film_lane == 0, 0.0, scaled * pltpu.roll(mid, 1, 1))
        right = jnp.where(film_lane == GRID - 1, 0.0, scaled * pltpu.roll(mid, GRID - 1, 1))
        rows = slice(8 * g, 8 * g + 8)
        weights[0, rows, :] = up
        weights[1, rows, :] = down
        weights[2, rows, :] = left
        weights[3, rows, :] = right
        weights[4, rows, :] = (up + down) + (left + right)

    def exchange(slot, g):
        top = 8 + 8 * g
        rows = slice(8 * g, 8 * g + 8)
        w = [weights[k, rows, :] for k in range(5)]
        magnet, result = [], []
        for c in range(3):
            mid = state[slot, c, top : top + 8, :]
            total = w[0] * state[slot, c, top - 1 : top + 7, :]
            total = total + w[1] * state[slot, c, top + 1 : top + 9, :]
            total = total + w[2] * pltpu.roll(mid, 1, 1)
            total = total + w[3] * pltpu.roll(mid, GRID - 1, 1)
            magnet.append(mid)
            result.append(total - w[4] * mid)
        return magnet, result

    def coarse_group(slot, g):
        magnet, effective = exchange(slot, g)
        rows = slice(8 * g, 8 * g + 8)
        effective = [effective[c] + field[c, rows, :] for c in range(3)]
        effective[2] = effective[2] - magnet[2]
        rate = torque(magnet, effective)
        return [magnet[c] + (FINE * step_time) * rate[c] for c in range(3)]

    def source_slot(n):
        return jnp.where(n == 0, 2, n % 2)

    def first_sweep(n, carry):
        for g in range(4):
            new = coarse_group(source_slot(n), g)
            for c in range(3):
                state[(n + 1) % 2, c, 8 + 8 * g : 16 + 8 * g, :] = new[c]
        return carry

    lax.fori_loop(0, slice_index, first_sweep, 0)
    start_slot = source_slot(slice_index)
    for g in (1, 2):
        new = coarse_group(start_slot, g)
        for c in range(3):
            coarse_end[c, 8 * g - 8 : 8 * g, :] = new[c]
    for c in range(3):
        start = state[start_slot, c, 16:32, :]
        base[c, :, :] = start
        slope[c, :, :] = jnp.zeros_like(start)
        state[0, c, 16:32, :] = start

    low_half = lax.broadcasted_iota(jnp.int32, (ROWS, 128), 1) < 64
    even_quarter = (lax.broadcasted_iota(jnp.int32, (128, 128), 1) // 32) % 2 == 0

    def partner(value):
        return jnp.where(even_quarter, pltpu.roll(value, 32, 1), pltpu.roll(value, 96, 1))

    def send_column(worker, target):
        return pltpu.make_async_remote_copy(
            src_ref=outgoing.at[worker],
            dst_ref=columns.at[pl.ds(pl.multiple_of(ROWS * place, ROWS), ROWS), :],
            send_sem=out_send, recv_sem=out_recv,
            device_id=device(slice_index, target), device_id_type=MESH,
        )

    def send_back(target):
        return pltpu.make_async_remote_copy(
            src_ref=answer.at[pl.ds(pl.multiple_of(ROWS * target, ROWS), ROWS), :],
            dst_ref=returned.at[rank],
            send_sem=back_send, recv_sem=back_recv,
            device_id=device(slice_index, target), device_id_type=MESH,
        )

    def planes_of(parts):
        return [(k, 1 if k == 1 else 0) for k in parts] + [(k, 0 if k == 1 else 1) for k in parts]

    def wait_bytes(ref, semaphore):
        pltpu.make_async_copy(ref, ref, semaphore).wait()

    def evaluation(e, carry):
        slot = e % 2
        for c in range(3):
            edges[c : c + 1, :] = state[0, c, 16:17, :]
            edges[3 + c : 4 + c, :] = state[0, c, 31:32, :]
        edge_copies = [
            pltpu.make_async_remote_copy(
                src_ref=edges.at[pl.ds(row, 3), :], dst_ref=edge_in.at[slot, side, pl.ds(row, 3), :],
                send_sem=edge_send.at[side], recv_sem=edge_recv.at[slot, side],
                device_id=device(slice_index, target), device_id_type=MESH,
            )
            for side, target, row in ((0, below, 3), (1, above, 0))
        ]
        for copy in edge_copies:
            copy.start()

        magnet = jnp.concatenate([state[0, c, 16:32, :] for c in range(3)], axis=0)
        high, low = split(magnet)
        stacked = jnp.concatenate([high, low], axis=0)
        for parts in ((2, 1, 3, 0),):
            for k in parts:
                part = (place_z // 2 + k) % 4
                cols = pl.ds(pl.multiple_of(256 * part, 256), 256)
                wide = dot(stacked, e1_high[:, cols])
                spectrum = wide[0:48] + wide[48:96] + dot(high, e1_low[:, cols])
                for half in range(2):
                    t = 2 * part + half
                    lanes = slice(128 * half, 128 * half + 128)
                    mx, my, mz = spectrum[0:16, lanes], spectrum[16:32, lanes], spectrum[32:48, lanes]
                    outgoing[2 * t] = jnp.where(low_half, mx, pltpu.roll(my, 64, 1))
                    outgoing[2 * t + 1] = jnp.where(low_half, pltpu.roll(mx, 64, 1), my)
                    outgoing[PAIRED + t] = mz
        for far in (4, 3, 2, 1, 0):
            for dy in (2, 1, -1, 0):
                for dz in (far, -far) if far in (1, 2, 3) else (far,):
                    sy = dy if dz >= 0 else -dy
                    if (dz, sy) != (0, 0):
                        plane = (place_z + dz) % 8
                        turn = (offset + sy - dz + 8) % 4

                        @pl.when(turn < 3)
                        def _(plane=plane, turn=turn, sy=sy):
                            send_column(number(plane, turn), 4 * plane + (place_y + sy) % 4).start()

        @pl.when(works)
        def _():
            columns[pl.ds(pl.multiple_of(ROWS * place, ROWS), ROWS), :] = outgoing[rank]

        for copy in edge_copies:
            copy.wait()
        for c in range(3):
            state[0, c, 15:16, :] = edge_in[slot, 0, 3 + c : 4 + c, :]
            state[0, c, 32:33, :] = edge_in[slot, 1, c : c + 1, :]
        for g in (1, 2):
            _, effective = exchange(0, g)
            for c in range(3):
                local_field[c, 8 * g - 8 : 8 * g, :] = effective[c] + field[c, 8 * g : 8 * g + 8, :]

        @pl.when(works)
        def _():
            wait_bytes(columns.at[pl.ds(0, ROWS * (SPACE - 1)), :], out_recv)
            column_high, column_low = split(columns[...])
            column_both = jnp.concatenate([column_high, column_low], axis=1)
            for part in range(4):
                rows = slice(256 * part, 256 * part + 256)
                wide = dot(e2_high[rows, :], column_both)
                spectrum = wide[:, 0:128] + wide[:, 128:256] + dot(e2_low[rows, :], column_high)
                spectrum = spectrum.reshape(4, 2, 32, 128)
                real = spectrum[:, 0].reshape(128, 128)
                imag = spectrum[:, 1].reshape(128, 128)
                diag = diagonal[rows, :].reshape(4, 2, 32, 128)
                mix = cross_term[128 * part : 128 * part + 128, :]
                real_out = diag[:, 0].reshape(128, 128) * real + mix * partner(imag)
                imag_out = diag[:, 1].reshape(128, 128) * imag - mix * partner(real)
                both = jnp.stack(
                    [real_out.reshape(4, 32, 128), imag_out.reshape(4, 32, 128)], axis=1
                ).reshape(256, 128)
                both_high, both_low = split(both)
                mixed[rows, 0:128] = both_high
                mixed[rows, 128:256] = both_low
            for parts in ((2,), (1, 3), (0,)):
                for k in parts:
                    rows = pl.ds(pl.multiple_of(128 * ((place_z // 2 + k) % 4), 128), 128)
                    wide = dot(e1_high[rows, :], mixed[...])
                    answer[rows, :] = wide[:, 0:128] + wide[:, 128:256] + dot(e1_low[rows, :], mixed[:, 0:128])
                for dy in (2, 1, -1, 0):
                    for k, half in planes_of(parts):
                        target = 4 * (2 * ((place_z // 2 + k) % 4) + half) + (place_y + dy) % 4
                        if k == 0 and dy == 0:

                            @pl.when(target != place)
                            def _(target=target):
                                send_back(target).start()

                        else:
                            send_back(target).start()

            returned[rank] = answer[pl.ds(pl.multiple_of(ROWS * place, ROWS), ROWS), :]
            wait_bytes(outgoing.at[pl.ds(0, WORKERS - 1)], out_send)
            wait_bytes(returned.at[pl.ds(0, WORKERS - 1)], back_recv)

        @pl.when(jnp.logical_not(works))
        def _():
            wait_bytes(outgoing, out_send)
            wait_bytes(returned, back_recv)

        parts = [[], [], []]
        for t in range(8):
            first, second = returned[2 * t], returned[2 * t + 1]
            parts[0].append(jnp.where(low_half, first, pltpu.roll(second, 64, 1)))
            parts[1].append(jnp.where(low_half, pltpu.roll(first, 64, 1), second))
            parts[2].append(returned[PAIRED + t])
        spectrum = jnp.concatenate([jnp.concatenate(part, axis=1) for part in parts], axis=0)
        spectrum_high, spectrum_low = split(spectrum)
        wide = dot(jnp.concatenate([spectrum_high, spectrum_low], axis=0), e2_high[...])
        demag = wide[0:48] + wide[48:96] + dot(spectrum_high, e2_low[...])

        corrects = slot == 1
        length = jnp.where(corrects, 0.5 * step_time, step_time)
        for g in range(2):
            rows = slice(8 * g, 8 * g + 8)
            here = [state[0, c, 16 + 8 * g : 24 + 8 * g, :] for c in range(3)]
            effective = [local_field[c, rows, :] + demag[16 * c + 8 * g : 16 * c + 8 * g + 8] for c in range(3)]
            rate = torque(here, effective)
            for c in range(3):
                start = base[c, rows, :]
                new = start + length * (slope[c, rows, :] + rate[c])
                state[0, c, 16 + 8 * g : 24 + 8 * g, :] = new
                slope[c, rows, :] = jnp.where(corrects, 0.0, rate[c])
                base[c, rows, :] = jnp.where(corrects, new, start)

        @pl.when(works)
        def _():
            wait_bytes(answer.at[pl.ds(0, ROWS * (SPACE - 1)), :], back_send)

        return carry

    lax.fori_loop(0, 2 * FINE, evaluation, 0)

    own = slice_index
    mate = own + 1 - 2 * core
    for c in range(3):
        jumps[own, c, 8:24, :] = state[0, c, 16:32, :] - coarse_end[c, :, :]

    def send_rows(i):
        return pltpu.make_async_remote_copy(
            src_ref=jumps.at[own, :, pl.ds(8, ROWS), :], dst_ref=jumps.at[own, :, pl.ds(8, ROWS), :],
            send_sem=gather_send.at[i], recv_sem=gather_recv.at[own],
            device_id=device(own + 2 * i, place), device_id_type=MESH,
        )

    def send_rims(i):
        n, depth = own - 2 * i, 2 * i + 1
        return [
            pltpu.make_async_remote_copy(
                src_ref=jumps.at[n, :, pl.ds(source_row, depth), :], dst_ref=jumps.at[n, :, pl.ds(landing_row, depth), :],
                send_sem=rim_send.at[n, side], recv_sem=rim_recv.at[n, side],
                device_id=device(slice_index, target), device_id_type=MESH,
            )
            for side, target, source_row, landing_row in ((0, below, 24 - depth, 8 - depth), (1, above, 8, 24))
        ]

    def send_mate(n):
        return pltpu.make_async_remote_copy(
            src_ref=jumps.at[n], dst_ref=jumps.at[n],
            send_sem=forward_send.at[n], recv_sem=forward_recv.at[n],
            device_id=device(mate, place), device_id_type=MESH,
        )

    def holds(i):
        return core == 0 if i == 0 else chip >= i

    def start_rims(i):
        @pl.when(holds(i))
        def _():
            if i > 0:
                wait_bytes(jumps.at[own - 2 * i, :, pl.ds(8, ROWS), :], gather_recv.at[own - 2 * i])
            for copy in send_rims(i):
                copy.start()

    def pass_on(i):
        @pl.when(holds(i))
        def _():
            for copy in send_rims(i):
                copy.wait_recv()
            send_mate(own - 2 * i).start()

    start_rims(0)
    for i in (2, 3, 1):

        @pl.when(chip + i < TM // 2)
        def _(i=i):
            send_rows(i).start()

    start_rims(1)
    start_rims(3)
    start_rims(2)
    pass_on(0)
    pass_on(1)
    pass_on(3)

    def second_sweep(n, carry):
        @pl.when((chip >= 2) & (n == 2 * chip - 4))
        def _():
            pass_on(2)

        @pl.when(n % 2 != core)
        def _():
            wait_bytes(jumps.at[n], forward_recv.at[n])

        for g in range(4):
            new = coarse_group(source_slot(n), g)
            for c in range(3):
                state[(n + 1) % 2, c, 8 + 8 * g : 16 + 8 * g, :] = new[c] + jumps[n, c, 8 * g : 8 * g + 8, :]
        return carry

    lax.fori_loop(0, own, second_sweep, 0)
    for g in (1, 2):
        new = coarse_group(source_slot(own), g)
        for c in range(3):
            out[c, 8 * g - 8 : 8 * g, :] = new[c] + jumps[own, c, 8 * g : 8 * g + 8, :]

    for i in range(4):

        @pl.when(holds(i))
        def _(i=i):
            for copy in send_rims(i):
                copy.wait_send()
            send_mate(own - 2 * i).wait_send()

        if i > 0:

            @pl.when(chip + i < TM // 2)
            def _(i=i):
                send_rows(i).wait_send()


def solution(mesh):
    tables = twiddle_tables()
    vmem = pltpu.VMEM
    dma = pltpu.SemaphoreType.DMA
    scratch = [
        *[vmem(table.shape, F32) for table in tables],
        vmem((3, 3, 48, GRID), F32),
        vmem((3, 32, GRID), F32),
        vmem((48, GRID), F32),
        vmem((5, 32, GRID), F32),
        vmem((GRID, LENGTH), BF16),
        vmem((GRID, LENGTH), BF16),
        vmem((LENGTH, GRID), BF16),
        vmem((LENGTH, GRID), BF16),
        vmem((LENGTH, 128), F32),
        vmem((GRID, 128), F32),
        vmem((WORKERS, ROWS, 128), F32),
        vmem((GRID, 128), F32),
        vmem((LENGTH, 256), BF16),
        vmem((GRID, 128), F32),
        vmem((WORKERS, ROWS, 128), F32),
        vmem((8, GRID), F32),
        vmem((2, 2, 8, GRID), F32),
        vmem((3, ROWS, GRID), F32),
        vmem((3, ROWS, GRID), F32),
        vmem((3, ROWS, GRID), F32),
        vmem((3, ROWS, GRID), F32),
        vmem((TM, 3, 32, GRID), F32),
        dma((7,)),
        dma((2, 3)),
        dma((2, 3)),
        dma((2,)),
        dma((2, 2)),
        dma,
        dma,
        dma,
        dma,
        dma((4,)),
        dma((TM,)),
        dma((TM, 2)),
        dma((TM, 2)),
        dma((TM,)),
        dma((TM,)),
    ]

    def shards(initial_state, applied_field, coupling):
        by_component = [jnp.transpose(value, (1, 0, 2)) for value in (initial_state, applied_field)]
        result = pl.pallas_call(
            kernel,
            out_shape=pltpu.VMEM((3, ROWS, GRID), F32),
            in_specs=[pl.BlockSpec(memory_space=pl.ANY)] * 7,
            out_specs=pl.BlockSpec(memory_space=pltpu.VMEM),
            scratch_shapes=scratch,
            compiler_params=pltpu.CompilerParams(collective_id=0, has_side_effects=True),
        )(*by_component, coupling, *[jnp.asarray(table) for table in tables])
        return jnp.transpose(result, (1, 0, 2))[None]

    return jax.shard_map(
        shards,
        mesh=mesh,
        in_specs=(P("space", None, None), P("space", None, None), P("space", None)),
        out_specs=P("tm", "space", None, None),
        check_vma=False,
    )
```
